8 devices in a mesh: dp: 2 (over z, y), sp: 4 (over x, core).
Axes of the slice: x: 2, y: 2, z: 1, core: 2. Of those that a mesh axis runs over, the one named last changes fastest.
Arguments:
- images: float32 [64, 512, 512, 3], P('dp', 'sp'), parts along dimension 0
- w_patch: bfloat16 [16, 16, 3, 1152], replicated
- b_patch: float32 [1152], replicated
- pos_embed: bfloat16 [1024, 1152], P('sp')
- ln1_gain: float32 [1152], replicated
- ln1_bias: float32 [1152], replicated
- w_qkv: bfloat16 [1152, 3, 16, 72], replicated
- b_qkv: float32 [3, 16, 72], replicated
- w_out: bfloat16 [16, 72, 1152], replicated
- b_out: float32 [1152], replicated
- ln2_gain: float32 [1152], replicated
- ln2_bias: float32 [1152], replicated
- w_fc1: bfloat16 [1152, 4304], replicated
- b_fc1: float32 [4304], replicated
- w_fc2: bfloat16 [4304, 1152], replicated
- b_fc2: float32 [1152], replicated
Outputs:
- output: bfloat16 [64, 1024, 1152], P('dp', 'sp'), parts along dimension 0
There are 2 independent parts. The reference program is written for one: setup_inputs(seed, part) draws one part's arguments, and reference() takes and returns one part's arrays. A program takes and returns all parts, laid end to end along the dimension named above; an argument that names none is the same for every part.
All inputs are finite; a program needn't handle non-finite values.
Results may differ from the reference program's by a relative error of at most 0.00841065.
Values are sent between devices in bfloat16 or wider.
A program may use at most 1 GiB of HBM per device.

```python
import jax
import jax.numpy as jnp
from jax import lax

B = 32
IMG = 512
PATCH = 16
D = 1152
HEADS = 16
HEAD = 72
FF = 4304

GRID = IMG // PATCH
TOKENS = GRID * GRID
PATCH_DIM = PATCH * PATCH * 3
LN_EPS = 1e-6


def draw_normal(rng_key, arr_shape, std_dev):
    return jax.random.normal(rng_key, arr_shape, jnp.float32) * std_dev


def smooth_images(base_key, num_images):
    key_freq, key_phase, key_amp, key_noise = jax.random.split(base_key, 4)
    wave_freq = jax.random.uniform(key_freq, (num_images, 8, 2), jnp.float32, -4.0, 4.0) * (2.0 * jnp.pi / IMG)
    wave_phase = jax.random.uniform(key_phase, (num_images, 8, 3), jnp.float32, 0.0, 2.0 * jnp.pi)
    wave_amp = draw_normal(key_amp, (num_images, 8, 3), 0.5)
    coords = jnp.arange(IMG, dtype=jnp.float32)
    row_angle = wave_freq[:, :, 0, None] * coords
    col_angle = wave_freq[:, :, 1, None, None] * coords[:, None] + wave_phase[:, :, None, :]
    waves = (jnp.einsum('nky,nkxc->nyxc', jnp.cos(row_angle), wave_amp[:, :, None, :] * jnp.cos(col_angle))
             - jnp.einsum('nky,nkxc->nyxc', jnp.sin(row_angle), wave_amp[:, :, None, :] * jnp.sin(col_angle)))
    return waves + draw_normal(key_noise, (num_images, IMG, IMG, 3), 0.2)


def setup_inputs(seed: int = 0, part: int = 0) -> dict:
    sub_keys = jax.random.split(jax.random.key(seed), 16)
    qk_gain = jnp.array([1.5, 1.5, 1.0], jnp.float32)[None, :, None, None]
    return {
        'images': smooth_images(jax.random.fold_in(sub_keys[0], part), B),
        'w_patch': draw_normal(sub_keys[1], (PATCH, PATCH, 3, D), PATCH_DIM ** -0.5).astype(jnp.bfloat16),
        'b_patch': draw_normal(sub_keys[2], (D,), 0.5),
        'pos_embed': draw_normal(sub_keys[3], (TOKENS, D), 1.0).astype(jnp.bfloat16),
        'ln1_gain': 1.0 + draw_normal(sub_keys[4], (D,), 0.2),
        'ln1_bias': draw_normal(sub_keys[5], (D,), 0.5),
        'w_qkv': (draw_normal(sub_keys[6], (D, 3, HEADS, HEAD), D ** -0.5) * qk_gain).astype(jnp.bfloat16),
        'b_qkv': draw_normal(sub_keys[7], (3, HEADS, HEAD), 0.5),
        'w_out': draw_normal(sub_keys[8], (HEADS, HEAD, D), 2.0 * D ** -0.5).astype(jnp.bfloat16),
        'b_out': draw_normal(sub_keys[9], (D,), 0.5),
        'ln2_gain': 1.0 + draw_normal(sub_keys[10], (D,), 0.2),
        'ln2_bias': draw_normal(sub_keys[11], (D,), 0.5),
        'w_fc1': draw_normal(sub_keys[12], (D, FF), D ** -0.5).astype(jnp.bfloat16),
        'b_fc1': draw_normal(sub_keys[13], (FF,), 0.5),
        'w_fc2': draw_normal(sub_keys[14], (FF, D), 1.5 * FF ** -0.5).astype(jnp.bfloat16),
        'b_fc2': draw_normal(sub_keys[15], (D,), 0.5),
    }


def layer_norm(x_in, ln_gain, ln_bias):
    row_mean = jnp.mean(x_in, axis=-1, keepdims=True)
    centered = x_in - row_mean
    variance = jnp.mean(centered * centered, axis=-1, keepdims=True)
    return centered * lax.rsqrt(variance + LN_EPS) * ln_gain + ln_bias


def reference(images, w_patch, b_patch, pos_embed, ln1_gain, ln1_bias, w_qkv, b_qkv, w_out, b_out, ln2_gain, ln2_bias, w_fc1, b_fc1, w_fc2, b_fc2):
    w_patch_flat = w_patch.reshape(PATCH_DIM, D)
    w_qkv_flat = w_qkv.reshape(D, 3 * D)
    b_qkv_flat = b_qkv.reshape(3 * D)
    w_out_flat = w_out.reshape(D, D)
    pos_f32 = pos_embed.astype(jnp.float32)

    def encode_image(single_image):
        pixels = single_image.astype(jnp.bfloat16).reshape(GRID, PATCH, GRID, PATCH, 3)
        patches = jnp.transpose(pixels, (0, 2, 1, 3, 4)).reshape(TOKENS, PATCH_DIM)
        patch_embed = jnp.dot(patches, w_patch_flat, preferred_element_type=jnp.float32)
        x_zero = (patch_embed + b_patch + pos_f32).astype(jnp.bfloat16)
        normed = layer_norm(x_zero.astype(jnp.float32), ln1_gain, ln1_bias).astype(jnp.bfloat16)
        qkv_proj = (jnp.dot(normed, w_qkv_flat, preferred_element_type=jnp.float32) + b_qkv_flat).astype(jnp.bfloat16)
        queries = qkv_proj[:, :D].reshape(GRID, GRID, HEADS, HEAD)
        keys_all = qkv_proj[:, D:2 * D].reshape(TOKENS, HEADS, HEAD).astype(jnp.float32)
        values_all = qkv_proj[:, 2 * D:].reshape(TOKENS, HEADS, HEAD).astype(jnp.float32)

        def attend_row(row_queries):
            scores = jnp.einsum('qhe,khe->hqk', row_queries.astype(jnp.float32), keys_all) * HEAD ** -0.5
            weights = jax.nn.softmax(scores, axis=-1).astype(jnp.bfloat16).astype(jnp.float32)
            return jnp.einsum('hqk,khe->qhe', weights, values_all).astype(jnp.bfloat16)

        attended = lax.map(attend_row, queries).reshape(TOKENS, D)
        residual = x_zero.astype(jnp.float32) + jnp.dot(attended, w_out_flat, preferred_element_type=jnp.float32) + b_out
        normed_two = layer_norm(residual, ln2_gain, ln2_bias).astype(jnp.bfloat16)
        hidden = jax.nn.gelu(jnp.dot(normed_two, w_fc1, preferred_element_type=jnp.float32) + b_fc1, approximate=True).astype(jnp.bfloat16)
        return (residual + jnp.dot(hidden, w_fc2, preferred_element_type=jnp.float32) + b_fc2).astype(jnp.bfloat16)

    return lax.map(encode_image, images)
```

```python
import functools
import jax
import jax.numpy as jnp
from jax import lax
from jax.experimental import pallas as pl
from jax.experimental.pallas import tpu as pltpu
from jax.sharding import PartitionSpec as P

LN_EPS = 1e-6
CHUNKS = (1, 2, 2, 2, 1)
MIB = 2 ** 20
F32, BF16 = jnp.float32, jnp.bfloat16


def dot(a, b):
    return jnp.dot(a, b, preferred_element_type=F32)


def widen(col, lanes):
    return jnp.concatenate([col] * (lanes // 128), axis=1)


def embed_kernel(idx_ref, i0, i1, i2, i3, perm_ref, wp_ref, bp_ref, pos_ref, o0, o1, o2, o3, xs):
    imgs = (i0, i1, i2, i3)
    outs = (o0, o1, o2, o3)
    zs = []
    for j in range(4):
        rows = []
        for k in range(4):
            for g in range(2):
                y = (4 * g + j) * 16
                for c in range(3):
                    rows.append(imgs[k][0, c, y:y + 16, :])
        zs.append(dot(jnp.concatenate(rows, axis=0).astype(BF16), perm_ref[j]))
    group = lax.broadcasted_iota(jnp.int32, (48, 128), 1) // 32
    for k in range(4):
        for g in range(2):
            r = (k * 2 + g) * 48
            for v in range(4):
                for u in range(4):
                    acc = zs[0][r:r + 48, 128 * v:128 * v + 128]
                    for j in range(1, 4):
                        acc = jnp.where(group == (u + j) % 4, zs[j][r:r + 48, 128 * v:128 * v + 128], acc)
                    if u:
                        acc = pltpu.roll(acc, 128 - 32 * u, 1)
                    px = 4 * v + u
                    xs[px * 48:px * 48 + 48, k * 256 + g * 128:k * 256 + g * 128 + 128] = acc.astype(BF16)
    step = 384

    def body(m, _):
        ms = pl.multiple_of(m * step, step)
        t = dot(wp_ref[pl.ds(ms, step), :], xs[...])
        t = t + widen(bp_ref[pl.ds(ms, step), :], 1024)
        p = pos_ref[pl.ds(ms, step), :].astype(F32)
        t = (t + jnp.concatenate([p] * 4, axis=1)).astype(BF16)
        for k in range(4):
            outs[k][0, pl.ds(ms, step), :] = t[:, k * 256:(k + 1) * 256]
        return 0

    lax.fori_loop(0, 1152 // step, body, 0)


def embed(idx, planes, perm, wp, bp, pos, n):
    d = wp.shape[0]

    def img(k):
        return pl.BlockSpec((1, 3, 128, 512), lambda i, idx, k=k: (idx[k] + i, 0, 0, 0))

    def whole(a):
        return pl.BlockSpec(a.shape, lambda i, idx: (0,) * a.ndim, pipeline_mode=pl.Buffered(1))

    return pl.pallas_call(
        embed_kernel,
        grid_spec=pltpu.PrefetchScalarGridSpec(
            num_scalar_prefetch=1, grid=(n,),
            in_specs=[img(0), img(1), img(2), img(3), whole(perm), whole(wp), whole(bp), whole(pos)],
            out_specs=[pl.BlockSpec((1, d, 256), lambda i, idx: (i, 0, 0))] * 4,
            scratch_shapes=[pltpu.VMEM((768, 1024), BF16)]),
        out_shape=[jax.ShapeDtypeStruct((n, d, 256), BF16)] * 4,
        name="embed",
        cost_estimate=pl.CostEstimate(flops=2 * n * 1024 * 768 * 1152, bytes_accessed=n * 6 * MIB, transcendentals=0),
        compiler_params=pltpu.CompilerParams(vmem_limit_bytes=56 * MIB),
    )(idx, planes, planes, planes, planes, perm, wp, bp, pos)


def normed(x, gain, bias):
    mean = jnp.mean(x, axis=0, keepdims=True)
    cen = x - mean
    var = jnp.mean(cen * cen, axis=0, keepdims=True)
    lanes = x.shape[1]
    return (cen * lax.rsqrt(var + LN_EPS) * widen(gain, lanes) + widen(bias, lanes)).astype(BF16)


def attn_kernel(x0, x1, x2, x3, w_ref, b_ref, g_ref, c_ref, o_ref, y1, qt, kn, vt, sa, sb):
    bands = (x0, x1, x2, x3)
    for k in range(4):
        for s in range(2):
            ln = slice(s * 128, s * 128 + 128)
            y1[:, k * 256 + s * 128:k * 256 + s * 128 + 128] = normed(bands[k][0, :, ln].astype(F32), g_ref[...], c_ref[...])
    zero8 = jnp.zeros((8, 1024), F32)
    for t in range(3):
        def proj(i, _, t=t):
            ms = pl.multiple_of(t * 1152 + i * 576, 576)
            acc = dot(w_ref[pl.ds(ms, 576), :], y1[...]) + widen(b_ref[pl.ds(ms, 576), :], 1024)
            for j in range(8):
                part = jnp.concatenate([acc[j * 72:j * 72 + 72], zero8], axis=0)
                if t == 0:
                    qt[i * 8 + j] = part.astype(BF16)
                elif t == 1:
                    kn[i * 8 + j] = part.T.astype(BF16)
                else:
                    vt[i * 8 + j] = part.astype(BF16)
            return 0
        lax.fori_loop(0, 2, proj, 0)
    scale = 1.4426950408889634 * 72 ** -0.5

    def score(h, ls, buf):
        s = dot(kn[h], qt[h, :, pl.ds(ls, 512)])
        buf[...] = s
        return jnp.max(s, axis=0, keepdims=True)

    def finish(h, buf, m):
        e = jnp.exp2((buf[...] - m) * scale)
        l = jnp.sum(e, axis=0, keepdims=True)
        return dot(vt[h], e.astype(BF16))[:72] * (1.0 / l)

    def tiles(i, m):
        hp = i // 2
        ls = pl.multiple_of((i % 2) * 512, 512)
        m1 = score(hp * 2 + 1, ls, sb)
        first = finish(hp * 2, sa, m)
        ni = jnp.minimum(i + 1, 15)
        m2 = score((ni // 2) * 2, pl.multiple_of((ni % 2) * 512, 512), sa)
        second = finish(hp * 2 + 1, sb, m1)
        pair = jnp.concatenate([first, second], axis=0).astype(BF16)
        o_ref[0, pl.ds(pl.multiple_of(hp * 144, 144), 144), pl.ds(ls, 512)] = pair
        return m2

    lax.fori_loop(0, 16, tiles, score(0, 0, sa))


def whole1(a):
    return pl.BlockSpec(a.shape, lambda i: (0,) * a.ndim, pipeline_mode=pl.Buffered(1))


def attention(xs, w, b, g, c):
    n, d, _ = xs[0].shape
    band = pl.BlockSpec((1, d, 256), lambda i: (i, 0, 0))
    return pl.pallas_call(
        attn_kernel, grid=(n,),
        in_specs=[band] * 4 + [whole1(w), whole1(b), whole1(g), whole1(c)],
        out_specs=pl.BlockSpec((1, d, 1024), lambda i: (i, 0, 0)),
        out_shape=jax.ShapeDtypeStruct((n, d, 1024), BF16),
        scratch_shapes=[pltpu.VMEM((d, 1024), BF16), pltpu.VMEM((16, 80, 1024), BF16), pltpu.VMEM((16, 1024, 80), BF16), pltpu.VMEM((16, 80, 1024), BF16),
                        pltpu.VMEM((1024, 512), F32), pltpu.VMEM((1024, 512), F32)],
        name="attn",
        cost_estimate=pl.CostEstimate(flops=n * 25 * 10 ** 9, bytes_accessed=n * 5 * MIB + 10 * MIB, transcendentals=0),
        compiler_params=pltpu.CompilerParams(vmem_limit_bytes=60 * MIB),
    )(*xs, w, b, g, c)


def mlp_kernel(a_ref, x0, x1, x2, x3, wo, bo, g_ref, c_ref, w1, b1, w2, b2, o0, o1, o2, o3, r, y2, hh):
    bands = (x0, x1, x2, x3)
    outs = (o0, o1, o2, o3)

    def proj(i, _):
        ms = pl.multiple_of(i * 576, 576)
        t = dot(wo[pl.ds(ms, 576), :], a_ref[0]) + widen(bo[pl.ds(ms, 576), :], 1024)
        for k in range(4):
            r[pl.ds(ms, 576), k * 256:(k + 1) * 256] = t[:, k * 256:(k + 1) * 256] + bands[k][0, pl.ds(ms, 576), :].astype(F32)
        return 0

    lax.fori_loop(0, 2, proj, 0)

    def norm(i, _):
        ls = pl.multiple_of(i * 128, 128)
        y2[:, pl.ds(ls, 128)] = normed(r[:, pl.ds(ls, 128)], g_ref[...], c_ref[...])
        return 0

    lax.fori_loop(0, 8, norm, 0)

    def up(i, _):
        ms = pl.multiple_of(i * 272, 272)
        z = dot(w1[pl.ds(ms, 272), :], y2[...]) + widen(b1[pl.ds(ms, 272), :], 1024)
        hh[pl.ds(ms, 272), :] = jax.nn.gelu(z, approximate=True).astype(BF16)
        return 0

    lax.fori_loop(0, 16, up, 0)

    def down(k, _):
        ls = pl.multiple_of(k * 256, 256)
        t = dot(w2[...], hh[:, pl.ds(ls, 256)]) + widen(b2[...], 256) + r[:, pl.ds(ls, 256)]
        t = t.T.astype(BF16)
        for j in range(4):
            @pl.when(k == j)
            def _():
                outs[j][0] = t
        return 0

    lax.fori_loop(0, 4, down, 0)


def mlp(att, xs, wo, bo, g, c, w1, b1, w2, b2):
    n, d, _ = xs[0].shape
    f = w1.shape[0]
    band = pl.BlockSpec((1, d, 256), lambda i: (i, 0, 0))
    ws = (wo, bo, g, c, w1, b1, w2, b2)
    return pl.pallas_call(
        mlp_kernel, grid=(n,),
        in_specs=[pl.BlockSpec((1, d, 1024), lambda i: (i, 0, 0))] + [band] * 4 + [whole1(a) for a in ws],
        out_specs=[pl.BlockSpec((1, 256, d), lambda i: (i, 0, 0))] * 4,
        out_shape=[jax.ShapeDtypeStruct((n, 256, d), BF16)] * 4,
        scratch_shapes=[pltpu.VMEM((d, 1024), F32), pltpu.VMEM((d, 1024), BF16), pltpu.VMEM((f, 1024), BF16)],
        name="mlp",
        cost_estimate=pl.CostEstimate(flops=n * 26 * 10 ** 9, bytes_accessed=n * 8 * MIB + 23 * MIB, transcendentals=0),
        compiler_params=pltpu.CompilerParams(vmem_limit_bytes=63 * MIB),
    )(att, *xs, *ws)


def column(v, pad=0):
    v = jnp.pad(v, (0, pad)) if pad else v
    return jnp.broadcast_to(v[:, None], (v.shape[0], 128))


def solution(mesh):
    sp = mesh.shape['sp']

    def device_step(images, w_patch, b_patch, pos_embed, ln1_gain, ln1_bias, w_qkv, b_qkv, w_out, b_out, ln2_gain, ln2_bias, w_fc1, b_fc1, w_fc2, b_fc2):
        me = lax.axis_index('sp')
        d = w_patch.shape[3]
        per = images.shape[0] // sp
        planes = jnp.transpose(images, (0, 3, 1, 2))
        x = jnp.arange(512)[:, None]
        o = jnp.arange(512)[None, :]
        px, gx = x % 16, x // 16
        perm = jnp.stack([(o == 128 * (px // 4) + 32 * ((px % 4 + j) % 4) + gx) for j in range(4)]).astype(BF16)
        wp = jnp.transpose(w_patch, (3, 1, 2, 0)).reshape(d, 768)
        pos = pos_embed.T
        bp = column(b_patch)
        wq = jnp.transpose(w_qkv, (1, 2, 3, 0)).reshape(3 * d, d)
        bq = column(b_qkv.reshape(3 * d))
        g1, c1 = column(ln1_gain), column(ln1_bias)
        wo = w_out.reshape(d, d).T
        bo, g2, c2 = column(b_out), column(ln2_gain), column(ln2_bias)
        pad = 4352 - w_fc1.shape[1]
        w1 = jnp.pad(w_fc1.T, ((0, pad), (0, 0)))
        b1 = column(b_fc1, pad)
        w2 = jnp.pad(w_fc2.T, ((0, 0), (0, pad)))
        b2 = column(b_fc2)

        def swap(a, k):
            return lax.ppermute(a, 'sp', [(i, i ^ k) for i in range(sp)]) if k else a

        peers = [me ^ k for k in range(sp)]
        starts = [sum(CHUNKS[:c]) for c in range(len(CHUNKS))]
        got = []
        for c, n in enumerate(CHUNKS):
            idx = jnp.stack([p * per + starts[c] for p in peers]).astype(jnp.int32)
            mine = embed(idx, planes, perm, wp, bp, pos, n)
            got.append([swap(a, k) for k, a in enumerate(mine)])
        out = pl.pallas_call(lambda o_ref: None, out_specs=pl.BlockSpec(memory_space=pl.ANY), name="blank",
                             out_shape=jax.ShapeDtypeStruct((images.shape[0], 256, d), BF16))()
        for c, n in enumerate(CHUNKS):
            att = attention(got[c], wq, bq, g1, c1)
            res = mlp(att, got[c], wo, bo, g2, c2, w1, b1, w2, b2)
            for k in range(sp):
                back = swap(res[k], k)
                out = lax.dynamic_update_slice(out, back, (peers[k] * per + starts[c], 0, 0))
        return out

    in_specs = (P('dp', 'sp', None, None), P(), P(), P('sp', None)) + (P(),) * 12
    return jax.shard_map(device_step, mesh=mesh, in_specs=in_specs, out_specs=P('dp', 'sp', None), check_vma=False)
```

```python
import functools
import jax
import jax.numpy as jnp
from jax import lax
from jax.experimental import pallas as pl
from jax.experimental.pallas import tpu as pltpu
from jax.sharding import PartitionSpec as P

LN_EPS = 1e-6
CHUNKS = (1, 2, 2, 2, 1)
MIB = 2 ** 20
F32, BF16 = jnp.float32, jnp.bfloat16


def dot(a, b):
    return jnp.dot(a, b, preferred_element_type=F32)


def widen(col, lanes):
    return jnp.concatenate([col] * (lanes // 128), axis=1)


def embed_kernel(idx_ref, i0, i1, i2, i3, perm_ref, wp_ref, bp_ref, pos_ref, o0, o1, o2, o3, xs):
    imgs = (i0, i1, i2, i3)
    outs = (o0, o1, o2, o3)
    zs = []
    for j in range(4):
        rows = []
        for k in range(4):
            for g in range(2):
                y = (4 * g + j) * 16
                for c in range(3):
                    rows.append(imgs[k][0, c, y:y + 16, :])
        zs.append(dot(jnp.concatenate(rows, axis=0).astype(BF16), perm_ref[j]))
    group = lax.broadcasted_iota(jnp.int32, (48, 128), 1) // 32
    for k in range(4):
        for g in range(2):
            r = (k * 2 + g) * 48
            for v in range(4):
                for u in range(4):
                    acc = zs[0][r:r + 48, 128 * v:128 * v + 128]
                    for j in range(1, 4):
                        acc = jnp.where(group == (u + j) % 4, zs[j][r:r + 48, 128 * v:128 * v + 128], acc)
                    if u:
                        acc = pltpu.roll(acc, 128 - 32 * u, 1)
                    px = 4 * v + u
                    xs[px * 48:px * 48 + 48, k * 256 + g * 128:k * 256 + g * 128 + 128] = acc.astype(BF16)
    step = 384

    def body(m, _):
        ms = pl.multiple_of(m * step, step)
        t = dot(wp_ref[pl.ds(ms, step), :], xs[...])
        t = t + widen(bp_ref[pl.ds(ms, step), :], 1024)
        p = pos_ref[pl.ds(ms, step), :].astype(F32)
        t = (t + jnp.concatenate([p] * 4, axis=1)).astype(BF16)
        for k in range(4):
            outs[k][0, pl.ds(ms, step), :] = t[:, k * 256:(k + 1) * 256]
        return 0

    lax.fori_loop(0, 1152 // step, body, 0)


def embed(idx, planes, perm, wp, bp, pos, n):
    d = wp.shape[0]

    def img(k):
        return pl.BlockSpec((1, 3, 128, 512), lambda i, idx, k=k: (idx[k] + i, 0, 0, 0))

    def whole(a):
        return pl.BlockSpec(a.shape, lambda i, idx: (0,) * a.ndim, pipeline_mode=pl.Buffered(1))

    return pl.pallas_call(
        embed_kernel,
        grid_spec=pltpu.PrefetchScalarGridSpec(
            num_scalar_prefetch=1, grid=(n,),
            in_specs=[img(0), img(1), img(2), img(3), whole(perm), whole(wp), whole(bp), whole(pos)],
            out_specs=[pl.BlockSpec((1, d, 256), lambda i, idx: (i, 0, 0))] * 4,
            scratch_shapes=[pltpu.VMEM((768, 1024), BF16)]),
        out_shape=[jax.ShapeDtypeStruct((n, d, 256), BF16)] * 4,
        name="embed",
        cost_estimate=pl.CostEstimate(flops=2 * n * 1024 * 768 * 1152, bytes_accessed=n * 6 * MIB, transcendentals=0),
        compiler_params=pltpu.CompilerParams(vmem_limit_bytes=56 * MIB),
    )(idx, planes, planes, planes, planes, perm, wp, bp, pos)


def row_mean(x, parts=8):
    rows = x.shape[0] // parts
    sums = [jnp.sum(x[i * rows:(i + 1) * rows].reshape(rows // 8, 8, x.shape[1]), axis=0) for i in range(parts)]
    while len(sums) > 1:
        sums = [p + q for p, q in zip(sums[::2], sums[1::2])]
    return jnp.sum(sums[0], axis=0, keepdims=True) * (1.0 / x.shape[0])


def normed(x, gain, bias):
    cen = x - row_mean(x)
    lanes = x.shape[1]
    return (cen * lax.rsqrt(row_mean(cen * cen) + LN_EPS) * widen(gain, lanes) + widen(bias, lanes)).astype(BF16)


def gelu(z):
    c = 0.7978845608028654
    half = 0.5 * z
    return half + half * jnp.tanh(z * (c + (c * 0.044715) * (z * z)))


ANY = pl.BlockSpec(memory_space=pl.ANY)


def attn_kernel(x0, x1, x2, x3, w_hbm, b_hbm, g_ref, c_ref, o_ref, y1, qt, kn, vt, sa, sb, w_ref, b_ref, sems):
    bands = (x0, x1, x2, x3)
    first = pl.program_id(0) == 0
    loads = [pltpu.make_async_copy(b_hbm, b_ref, sems.at[3])]
    for t in range(3):
        rows = pl.ds(t * 1152, 1152)
        loads.append(pltpu.make_async_copy(w_hbm.at[rows, :], w_ref.at[rows, :], sems.at[t]))

    @pl.when(first)
    def _():
        for cp in loads:
            cp.start()

    for k in range(4):
        y1[:, k * 256:k * 256 + 256] = normed(bands[k][0].astype(F32), g_ref[...], c_ref[...])
    zero8 = jnp.zeros((8, 1024), F32)
    for t in range(3):
        @pl.when(first)
        def _(t=t):
            if t == 0:
                loads[0].wait()
            loads[t + 1].wait()

        def proj(i, _, t=t):
            ms = pl.multiple_of(t * 1152 + i * 576, 576)
            acc = dot(w_ref[pl.ds(ms, 576), :], y1[...]) + widen(b_ref[pl.ds(ms, 576), :], 1024)
            for j in range(8):
                part = jnp.concatenate([acc[j * 72:j * 72 + 72], zero8], axis=0)
                if t == 0:
                    qt[i * 8 + j] = part.astype(BF16)
                elif t == 1:
                    kn[i * 8 + j] = part.T.astype(BF16)
                else:
                    vt[i * 8 + j] = part.astype(BF16)
            return 0
        lax.fori_loop(0, 2, proj, 0)
    scale = 1.4426950408889634 * 72 ** -0.5

    def score(h, ls, buf):
        s = dot(kn[h], qt[h, :, pl.ds(ls, 512)])
        buf[...] = s
        return jnp.max(s, axis=0, keepdims=True)

    def finish(h, buf, m):
        e = jnp.exp2((buf[...] - m) * scale)
        l = jnp.sum(e, axis=0, keepdims=True)
        return dot(vt[h], e.astype(BF16))[:72] * (1.0 / l)

    def tiles(i, m):
        hp = i // 2
        ls = pl.multiple_of((i % 2) * 512, 512)
        m1 = score(hp * 2 + 1, ls, sb)
        first = finish(hp * 2, sa, m)
        ni = jnp.minimum(i + 1, 15)
        m2 = score((ni // 2) * 2, pl.multiple_of((ni % 2) * 512, 512), sa)
        second = finish(hp * 2 + 1, sb, m1)
        pair = jnp.concatenate([first, second], axis=0).astype(BF16)
        o_ref[0, pl.ds(pl.multiple_of(hp * 144, 144), 144), pl.ds(ls, 512)] = pair
        return m2

    lax.fori_loop(0, 16, tiles, score(0, 0, sa))


def whole1(a):
    return pl.BlockSpec(a.shape, lambda i: (0,) * a.ndim, pipeline_mode=pl.Buffered(1))


def attention(xs, w, b, g, c):
    n, d, _ = xs[0].shape
    band = pl.BlockSpec((1, d, 256), lambda i: (i, 0, 0))
    return pl.pallas_call(
        attn_kernel, grid=(n,),
        in_specs=[band] * 4 + [ANY, ANY, whole1(g), whole1(c)],
        out_specs=pl.BlockSpec((1, d, 1024), lambda i: (i, 0, 0)),
        out_shape=jax.ShapeDtypeStruct((n, d, 1024), BF16),
        scratch_shapes=[pltpu.VMEM((d, 1024), BF16), pltpu.VMEM((16, 80, 1024), BF16), pltpu.VMEM((16, 1024, 80), BF16), pltpu.VMEM((16, 80, 1024), BF16),
                        pltpu.VMEM((1024, 512), F32), pltpu.VMEM((1024, 512), F32),
                        pltpu.VMEM(w.shape, BF16), pltpu.VMEM(b.shape, F32), pltpu.SemaphoreType.DMA((4,))],
        name="attn",
        cost_estimate=pl.CostEstimate(flops=n * 25 * 10 ** 9, bytes_accessed=n * 5 * MIB + 10 * MIB, transcendentals=0),
        compiler_params=pltpu.CompilerParams(vmem_limit_bytes=60 * MIB),
    )(*xs, w, b, g, c)


def mlp_kernel(a_ref, x0, x1, x2, x3, wo_hbm, bo, g_ref, c_ref, w1_hbm, b1_hbm, w2_hbm, b2, o0, o1, o2, o3, r, y2, hh, wo, w1, b1, w2, sems):
    bands = (x0, x1, x2, x3)
    outs = (o0, o1, o2, o3)
    first = pl.program_id(0) == 0
    ff = w1_hbm.shape[0]
    full = w1.shape[0]
    tile = full // 4
    ups = []
    for j in range(4):
        rows = pl.ds(j * tile, min(tile, ff - j * tile))
        ups.append(pltpu.make_async_copy(w1_hbm.at[rows, :], w1.at[rows, :], sems.at[j]))
    load_o = pltpu.make_async_copy(wo_hbm, wo, sems.at[4])
    load_b = pltpu.make_async_copy(b1_hbm, b1, sems.at[5])
    load_2 = pltpu.make_async_copy(w2_hbm, w2, sems.at[6])

    @pl.when(first)
    def _():
        load_o.start()
        load_b.start()
        for cp in ups:
            cp.start()
        load_2.start()
        w1[ff:full, :] = jnp.zeros((full - ff, w1.shape[1]), BF16)
        load_o.wait()

    def proj(i, _):
        ms = pl.multiple_of(i * 576, 576)
        t = dot(wo[pl.ds(ms, 576), :], a_ref[0]) + widen(bo[pl.ds(ms, 576), :], 1024)
        for k in range(4):
            r[pl.ds(ms, 576), k * 256:(k + 1) * 256] = t[:, k * 256:(k + 1) * 256] + bands[k][0, pl.ds(ms, 576), :].astype(F32)
        return 0

    lax.fori_loop(0, 2, proj, 0)

    def norm(i, _):
        ls = pl.multiple_of(i * 256, 256)
        y2[:, pl.ds(ls, 256)] = normed(r[:, pl.ds(ls, 256)], g_ref[...], c_ref[...])
        return 0

    lax.fori_loop(0, 4, norm, 0)

    @pl.when(first)
    def _():
        load_b.wait()

    def up(i, _):
        for j in range(4):
            @pl.when(first & (i == 2 * j))
            def _(j=j):
                ups[j].wait()
        ms = pl.multiple_of(i * (tile // 2), tile // 2)
        z = dot(w1[pl.ds(ms, tile // 2), :], y2[...]) + widen(b1[pl.ds(ms, tile // 2), :], 1024)
        hh[pl.ds(ms, tile // 2), :] = gelu(z).astype(BF16)
        return 0

    lax.fori_loop(0, 8, up, 0)

    @pl.when(first)
    def _():
        load_2.wait()

    def down(k, _):
        ls = pl.multiple_of(k * 256, 256)
        t = dot(w2[...], hh[:, pl.ds(ls, 256)]) + widen(b2[...], 256) + r[:, pl.ds(ls, 256)]
        t = t.astype(BF16).T
        for j in range(4):
            @pl.when(k == j)
            def _():
                outs[j][0] = t
        return 0

    lax.fori_loop(0, 4, down, 0)


def mlp(att, xs, wo, bo, g, c, w1, b1, w2, b2):
    n, d, _ = xs[0].shape
    f = w2.shape[1]
    band = pl.BlockSpec((1, d, 256), lambda i: (i, 0, 0))
    return pl.pallas_call(
        mlp_kernel, grid=(n,),
        in_specs=[pl.BlockSpec((1, d, 1024), lambda i: (i, 0, 0))] + [band] * 4 + [ANY, whole1(bo), whole1(g), whole1(c), ANY, ANY, ANY, whole1(b2)],
        out_specs=[pl.BlockSpec((1, 256, d), lambda i: (i, 0, 0))] * 4,
        out_shape=[jax.ShapeDtypeStruct((n, 256, d), BF16)] * 4,
        scratch_shapes=[pltpu.VMEM((d, 1024), F32), pltpu.VMEM((d, 1024), BF16), pltpu.VMEM((f, 1024), BF16),
                        pltpu.VMEM((d, d), BF16), pltpu.VMEM((f, d), BF16), pltpu.VMEM((f, 128), F32), pltpu.VMEM((d, f), BF16),
                        pltpu.SemaphoreType.DMA((7,))],
        name="mlp",
        cost_estimate=pl.CostEstimate(flops=n * 26 * 10 ** 9, bytes_accessed=n * 8 * MIB + 23 * MIB, transcendentals=0),
        compiler_params=pltpu.CompilerParams(vmem_limit_bytes=63 * MIB),
    )(att, *xs, wo, bo, g, c, w1, b1, w2, b2)


def flip_kernel(w_ref, o_ref, *, rows):
    at = pl.program_id(0) * w_ref.shape[0] + lax.broadcasted_iota(jnp.int32, w_ref.shape, 0)
    o_ref[...] = jnp.where(at < rows, w_ref[...], jnp.zeros_like(w_ref)).T


def flip(w, full, block):
    rows, d = w.shape
    return pl.pallas_call(
        functools.partial(flip_kernel, rows=rows), grid=(full // block,),
        in_specs=[pl.BlockSpec((block, d), lambda i: (i, 0))],
        out_specs=pl.BlockSpec((d, block), lambda i: (0, i)),
        out_shape=jax.ShapeDtypeStruct((d, full), BF16), name="flip",
        cost_estimate=pl.CostEstimate(flops=2 * 10 ** 9, bytes_accessed=20 * MIB, transcendentals=0),
    )(w)


def place_kernel(*refs, slots):
    n = len(slots)
    idx, parts, out, buf, sems = refs[0], refs[1:1 + n], refs[-3], refs[-2], refs[-1]
    copies = []
    at = 0
    for ref, (k, start) in zip(parts, slots):
        m = ref.shape[0]
        here = buf.at[pl.ds(at, m)]
        pull = pltpu.make_async_copy(ref, here, sems.at[0, len(copies)])
        push = pltpu.make_async_copy(here, out.at[pl.ds(idx[k] + start, m)], sems.at[1, len(copies)])
        copies.append((pull, push))
        pull.start()
        at += m
    for pull, push in copies:
        pull.wait()
        push.start()
    for _, push in copies:
        push.wait()


def place(idx, parts, slots, out_shape, base=None):
    n = len(parts)
    total = sum(p.shape[0] for p in parts)
    return pl.pallas_call(
        functools.partial(place_kernel, slots=slots),
        in_specs=[pl.BlockSpec(memory_space=pltpu.SMEM)] + [ANY] * (n + (base is not None)),
        out_specs=ANY, out_shape=out_shape, name="place",
        scratch_shapes=[pltpu.VMEM((total,) + parts[0].shape[1:], BF16), pltpu.SemaphoreType.DMA((2, n))],
        input_output_aliases={n + 1: 0} if base is not None else {},
        cost_estimate=pl.CostEstimate(flops=10 ** 9, bytes_accessed=2 * total * 589824, transcendentals=0),
        compiler_params=pltpu.CompilerParams(vmem_limit_bytes=40 * MIB),
    )(idx, *parts, *([base] if base is not None else []))


def column(v, pad=0):
    v = jnp.pad(v, (0, pad)) if pad else v
    return jnp.broadcast_to(v[:, None], (v.shape[0], 128))


def solution(mesh):
    sp = mesh.shape['sp']

    def device_step(images, w_patch, b_patch, pos_embed, ln1_gain, ln1_bias, w_qkv, b_qkv, w_out, b_out, ln2_gain, ln2_bias, w_fc1, b_fc1, w_fc2, b_fc2):
        me = lax.axis_index('sp')
        d = w_patch.shape[3]
        per = images.shape[0] // sp
        planes = jnp.transpose(images, (0, 3, 1, 2))
        x = jnp.arange(512)[:, None]
        o = jnp.arange(512)[None, :]
        px, gx = x % 16, x // 16
        perm = jnp.stack([(o == 128 * (px // 4) + 32 * ((px % 4 + j) % 4) + gx) for j in range(4)]).astype(BF16)
        wp = jnp.transpose(w_patch, (3, 1, 2, 0)).reshape(d, 768)
        pos = pos_embed.T
        bp = column(b_patch)
        wq = jnp.transpose(w_qkv, (1, 2, 3, 0)).reshape(3 * d, d)
        bq = column(b_qkv.reshape(3 * d))
        g1, c1 = column(ln1_gain), column(ln1_bias)
        wo = w_out.reshape(d, d).T
        bo, g2, c2 = column(b_out), column(ln2_gain), column(ln2_bias)
        pad = 4352 - w_fc1.shape[1]
        w1 = w_fc1.T
        b1 = column(b_fc1, pad)
        w2 = flip(w_fc2, 4352, 256)
        b2 = column(b_fc2)

        def swap(a, k):
            return lax.ppermute(a, 'sp', [(i, i ^ k) for i in range(sp)]) if k else a

        peers = [me ^ k for k in range(sp)]
        starts = [sum(CHUNKS[:c]) for c in range(len(CHUNKS))]
        got = []
        for c, n in enumerate(CHUNKS):
            idx = jnp.stack([p * per + starts[c] for p in peers]).astype(jnp.int32)
            mine = embed(idx, planes, perm, wp, bp, pos, n)
            got.append([swap(a, k) for k, a in enumerate(mine)])
        owner = jnp.stack([p * per for p in peers]).astype(jnp.int32)
        early, slots, res = [], [], None
        last = len(CHUNKS) - 1
        for c, n in enumerate(CHUNKS):
            xs = got[c]
            if c:
                own, _ = lax.optimization_barrier((xs[0], res[0]))
                xs = [own] + xs[1:]
            att = attention(xs, wq, bq, g1, c1)
            res = mlp(att, xs, wo, bo, g2, c2, w1, b1, w2, b2)
            back = [swap(a, k) for k, a in enumerate(res)]
            if c < last:
                early += back
                slots += [(k, starts[c]) for k in range(sp)]
        shape = jax.ShapeDtypeStruct((images.shape[0], 256, d), BF16)
        early, slots = early + back[:1], slots + [(0, starts[last])]
        out = place(owner, early, slots, shape)
        return place(owner, back[1:], [(k, starts[last]) for k in range(1, sp)], shape, out)

    in_specs = (P('dp', 'sp', None, None), P(), P(), P('sp', None)) + (P(),) * 12
    return jax.shard_map(device_step, mesh=mesh, in_specs=in_specs, out_specs=P('dp', 'sp', None), check_vma=False)
```

```python
import functools
import jax
import jax.numpy as jnp
from jax import lax
from jax.experimental import pallas as pl
from jax.experimental.pallas import tpu as pltpu
from jax.sharding import PartitionSpec as P

LN_EPS = 1e-6
GROUPS = (2, 6)
CHUNKS = (2, 2, 2, 1, 1)
MIB = 2 ** 20
F32, BF16 = jnp.float32, jnp.bfloat16


def dot(a, b):
    return jnp.dot(a, b, preferred_element_type=F32)


def widen(col, lanes):
    return jnp.concatenate([col] * (lanes // 128), axis=1)


def embed_kernel(idx_ref, i0, i1, i2, i3, perm_ref, wp_ref, bp_ref, pos_ref, o0, o1, o2, o3, xs):
    imgs = (i0, i1, i2, i3)
    outs = (o0, o1, o2, o3)
    zs = []
    for j in range(4):
        rows = []
        for k in range(4):
            for g in range(2):
                y = (4 * g + j) * 16
                for c in range(3):
                    rows.append(imgs[k][0, c, y:y + 16, :])
        zs.append(dot(jnp.concatenate(rows, axis=0).astype(BF16), perm_ref[j]))
    group = lax.broadcasted_iota(jnp.int32, (48, 128), 1) // 32
    for k in range(4):
        for g in range(2):
            r = (k * 2 + g) * 48
            for v in range(4):
                for u in range(4):
                    acc = zs[0][r:r + 48, 128 * v:128 * v + 128]
                    for j in range(1, 4):
                        acc = jnp.where(group == (u + j) % 4, zs[j][r:r + 48, 128 * v:128 * v + 128], acc)
                    if u:
                        acc = pltpu.roll(acc, 128 - 32 * u, 1)
                    px = 4 * v + u
                    xs[px * 48:px * 48 + 48, k * 256 + g * 128:k * 256 + g * 128 + 128] = acc.astype(BF16)
    step = 384

    def body(m, _):
        ms = pl.multiple_of(m * step, step)
        t = dot(wp_ref[pl.ds(ms, step), :], xs[...])
        t = t + widen(bp_ref[pl.ds(ms, step), :], 1024)
        p = pos_ref[pl.ds(ms, step), :].astype(F32)
        t = (t + jnp.concatenate([p] * 4, axis=1)).astype(BF16)
        for k in range(4):
            outs[k][0, pl.ds(ms, step), :] = t[:, k * 256:(k + 1) * 256]
        return 0

    lax.fori_loop(0, 1152 // step, body, 0)


def embed(idx, planes, perm, wp, bp, pos, n):
    d = wp.shape[0]

    def img(k):
        return pl.BlockSpec((1, 3, 128, 512), lambda i, idx, k=k: (idx[k] + i, 0, 0, 0))

    def whole(a):
        return pl.BlockSpec(a.shape, lambda i, idx: (0,) * a.ndim, pipeline_mode=pl.Buffered(1))

    return pl.pallas_call(
        embed_kernel,
        grid_spec=pltpu.PrefetchScalarGridSpec(
            num_scalar_prefetch=1, grid=(n,),
            in_specs=[img(0), img(1), img(2), img(3), whole(perm), whole(wp), whole(bp), whole(pos)],
            out_specs=[pl.BlockSpec((1, d, 256), lambda i, idx: (i, 0, 0))] * 4,
            scratch_shapes=[pltpu.VMEM((768, 1024), BF16)]),
        out_shape=[jax.ShapeDtypeStruct((n, d, 256), BF16)] * 4,
        name="embed",
        cost_estimate=pl.CostEstimate(flops=2 * n * 1024 * 768 * 1152, bytes_accessed=n * 6 * MIB, transcendentals=0),
        compiler_params=pltpu.CompilerParams(vmem_limit_bytes=56 * MIB),
    )(idx, planes, planes, planes, planes, perm, wp, bp, pos)


def row_mean(x, parts=8):
    rows = x.shape[0] // parts
    sums = [jnp.sum(x[i * rows:(i + 1) * rows].reshape(rows // 8, 8, x.shape[1]), axis=0) for i in range(parts)]
    while len(sums) > 1:
        sums = [p + q for p, q in zip(sums[::2], sums[1::2])]
    return jnp.sum(sums[0], axis=0, keepdims=True) * (1.0 / x.shape[0])


def normed(x, gain, bias):
    cen = x - row_mean(x)
    lanes = x.shape[1]
    return (cen * lax.rsqrt(row_mean(cen * cen) + LN_EPS) * widen(gain, lanes) + widen(bias, lanes)).astype(BF16)


def gelu(z):
    c = 0.7978845608028654
    half = 0.5 * z
    return half + half * jnp.tanh(z * (c + (c * 0.044715) * (z * z)))


ANY = pl.BlockSpec(memory_space=pl.ANY)


def attn_kernel(x0, x1, x2, x3, w_hbm, b_hbm, g_ref, c_ref, o_ref, y1, qt, kn, vt, sa, sb, w_ref, b_ref, sems):
    bands = (x0, x1, x2, x3)
    first = pl.program_id(0) == 0
    loads = [pltpu.make_async_copy(b_hbm, b_ref, sems.at[3])]
    for t in range(3):
        rows = pl.ds(t * 1152, 1152)
        loads.append(pltpu.make_async_copy(w_hbm.at[rows, :], w_ref.at[rows, :], sems.at[t]))

    @pl.when(first)
    def _():
        loads[0].start()
        loads[1].start()

    for k in range(4):
        y1[:, k * 256:k * 256 + 256] = normed(bands[k][0].astype(F32), g_ref[...], c_ref[...])
    zero8 = jnp.zeros((8, 1024), F32)
    for t in range(3):
        @pl.when(first)
        def _(t=t):
            if t == 0:
                loads[0].wait()
            loads[t + 1].wait()
            if t < 2:
                loads[t + 2].start()

        def proj(i, _, t=t):
            ms = pl.multiple_of(t * 1152 + i * 576, 576)
            acc = dot(w_ref[pl.ds(ms, 576), :], y1[...]) + widen(b_ref[pl.ds(ms, 576), :], 1024)
            for j in range(8):
                part = jnp.concatenate([acc[j * 72:j * 72 + 72], zero8], axis=0)
                if t == 0:
                    qt[i * 8 + j] = part.astype(BF16)
                elif t == 1:
                    kn[i * 8 + j] = part.T.astype(BF16)
                else:
                    vt[i * 8 + j] = part.astype(BF16)
            return 0
        lax.fori_loop(0, 2, proj, 0)
    scale = 1.4426950408889634 * 72 ** -0.5

    def score(h, ls, buf):
        s = dot(kn[h], qt[h, :, pl.ds(ls, 512)])
        buf[...] = s
        return jnp.max(s, axis=0, keepdims=True)

    def finish(h, buf, m):
        e = jnp.exp2((buf[...] - m) * scale)
        l = jnp.sum(e, axis=0, keepdims=True)
        return dot(vt[h], e.astype(BF16))[:72] * (1.0 / l)

    def tiles(i, m):
        hp = i // 2
        ls = pl.multiple_of((i % 2) * 512, 512)
        m1 = score(hp * 2 + 1, ls, sb)
        first = finish(hp * 2, sa, m)
        ni = jnp.minimum(i + 1, 15)
        m2 = score((ni // 2) * 2, pl.multiple_of((ni % 2) * 512, 512), sa)
        second = finish(hp * 2 + 1, sb, m1)
        pair = jnp.concatenate([first, second], axis=0).astype(BF16)
        o_ref[0, pl.ds(pl.multiple_of(hp * 144, 144), 144), pl.ds(ls, 512)] = pair
        return m2

    lax.fori_loop(0, 16, tiles, score(0, 0, sa))


def whole1(a):
    return pl.BlockSpec(a.shape, lambda i: (0,) * a.ndim, pipeline_mode=pl.Buffered(1))


def attention(xs, at, n, w, b, g, c):
    d = xs[0].shape[1]
    band = pl.BlockSpec((1, d, 256), lambda i: (i + at, 0, 0))
    return pl.pallas_call(
        attn_kernel, grid=(n,),
        in_specs=[band] * 4 + [ANY, ANY, whole1(g), whole1(c)],
        out_specs=pl.BlockSpec((1, d, 1024), lambda i: (i, 0, 0)),
        out_shape=jax.ShapeDtypeStruct((n, d, 1024), BF16),
        scratch_shapes=[pltpu.VMEM((d, 1024), BF16), pltpu.VMEM((16, 80, 1024), BF16), pltpu.VMEM((16, 1024, 80), BF16), pltpu.VMEM((16, 80, 1024), BF16),
                        pltpu.VMEM((1024, 512), F32), pltpu.VMEM((1024, 512), F32),
                        pltpu.VMEM(w.shape, BF16), pltpu.VMEM(b.shape, F32), pltpu.SemaphoreType.DMA((4,))],
        name="attn",
        cost_estimate=pl.CostEstimate(flops=n * 25 * 10 ** 9, bytes_accessed=n * 5 * MIB + 10 * MIB, transcendentals=0),
        compiler_params=pltpu.CompilerParams(vmem_limit_bytes=60 * MIB),
    )(*xs, w, b, g, c)


def mlp_kernel(a_ref, x0, x1, x2, x3, wo_hbm, bo, g_ref, c_ref, w1_hbm, b1_hbm, w2_hbm, b2, o0, o1, o2, o3, r, y2, hh, wo, w1, b1, w2, sems):
    bands = (x0, x1, x2, x3)
    outs = (o0, o1, o2, o3)
    first = pl.program_id(0) == 0
    ff = w1_hbm.shape[0]
    full = w1.shape[0]
    tile = full // 4
    ups = []
    for j in range(4):
        rows = pl.ds(j * tile, min(tile, ff - j * tile))
        ups.append(pltpu.make_async_copy(w1_hbm.at[rows, :], w1.at[rows, :], sems.at[j]))
    load_o = pltpu.make_async_copy(wo_hbm, wo, sems.at[4])
    load_b = pltpu.make_async_copy(b1_hbm, b1, sems.at[5])
    load_2 = pltpu.make_async_copy(w2_hbm, w2, sems.at[6])

    @pl.when(first)
    def _():
        load_o.start()
        w1[ff:full, :] = jnp.zeros((full - ff, w1.shape[1]), BF16)
        load_o.wait()
        load_b.start()
        ups[0].start()
        ups[1].start()

    def proj(i, _):
        ms = pl.multiple_of(i * 576, 576)
        t = dot(wo[pl.ds(ms, 576), :], a_ref[0]) + widen(bo[pl.ds(ms, 576), :], 1024)
        for k in range(4):
            r[pl.ds(ms, 576), k * 256:(k + 1) * 256] = t[:, k * 256:(k + 1) * 256] + bands[k][0, pl.ds(ms, 576), :].astype(F32)
        return 0

    lax.fori_loop(0, 2, proj, 0)

    def norm(i, _):
        ls = pl.multiple_of(i * 256, 256)
        y2[:, pl.ds(ls, 256)] = normed(r[:, pl.ds(ls, 256)], g_ref[...], c_ref[...])
        return 0

    lax.fori_loop(0, 4, norm, 0)

    @pl.when(first)
    def _():
        load_b.wait()

    def up(i, _):
        for j in range(4):
            @pl.when(first & (i == 2 * j))
            def _(j=j):
                ups[j].wait()
                if j < 2:
                    ups[j + 2].start()
                elif j == 2:
                    load_2.start()
        ms = pl.multiple_of(i * (tile // 2), tile // 2)
        z = dot(w1[pl.ds(ms, tile // 2), :], y2[...]) + widen(b1[pl.ds(ms, tile // 2), :], 1024)
        hh[pl.ds(ms, tile // 2), :] = gelu(z).astype(BF16)
        return 0

    lax.fori_loop(0, 8, up, 0)

    @pl.when(first)
    def _():
        load_2.wait()

    def down(k, _):
        ls = pl.multiple_of(k * 256, 256)
        t = dot(w2[...], hh[:, pl.ds(ls, 256)]) + widen(b2[...], 256) + r[:, pl.ds(ls, 256)]
        t = t.astype(BF16).T
        for j in range(4):
            @pl.when(k == j)
            def _():
                outs[j][0] = t
        return 0

    lax.fori_loop(0, 4, down, 0)


def mlp(att, xs, at, wo, bo, g, c, w1, b1, w2, b2):
    n, d, _ = att.shape
    f = w2.shape[1]
    band = pl.BlockSpec((1, d, 256), lambda i: (i + at, 0, 0))
    return pl.pallas_call(
        mlp_kernel, grid=(n,),
        in_specs=[pl.BlockSpec((1, d, 1024), lambda i: (i, 0, 0))] + [band] * 4 + [ANY, whole1(bo), whole1(g), whole1(c), ANY, ANY, ANY, whole1(b2)],
        out_specs=[pl.BlockSpec((1, 256, d), lambda i: (i, 0, 0))] * 4,
        out_shape=[jax.ShapeDtypeStruct((n, 256, d), BF16)] * 4,
        scratch_shapes=[pltpu.VMEM((d, 1024), F32), pltpu.VMEM((d, 1024), BF16), pltpu.VMEM((f, 1024), BF16),
                        pltpu.VMEM((d, d), BF16), pltpu.VMEM((f, d), BF16), pltpu.VMEM((f, 128), F32), pltpu.VMEM((d, f), BF16),
                        pltpu.SemaphoreType.DMA((7,))],
        name="mlp",
        cost_estimate=pl.CostEstimate(flops=n * 26 * 10 ** 9, bytes_accessed=n * 8 * MIB + 23 * MIB, transcendentals=0),
        compiler_params=pltpu.CompilerParams(vmem_limit_bytes=63 * MIB),
    )(att, *xs, wo, bo, g, c, w1, b1, w2, b2)


def flip_kernel(w_ref, o_ref, *, rows):
    at = pl.program_id(0) * w_ref.shape[0] + lax.broadcasted_iota(jnp.int32, w_ref.shape, 0)
    o_ref[...] = jnp.where(at < rows, w_ref[...], jnp.zeros_like(w_ref)).T


def flip(w, full, block):
    rows, d = w.shape
    return pl.pallas_call(
        functools.partial(flip_kernel, rows=rows), grid=(full // block,),
        in_specs=[pl.BlockSpec((block, d), lambda i: (i, 0))],
        out_specs=pl.BlockSpec((d, block), lambda i: (0, i)),
        out_shape=jax.ShapeDtypeStruct((d, full), BF16), name="flip",
        cost_estimate=pl.CostEstimate(flops=2 * 10 ** 9, bytes_accessed=20 * MIB, transcendentals=0),
    )(w)


def place_kernel(*refs, slots):
    n = len(slots)
    idx, parts, out, buf, sems = refs[0], refs[1:1 + n], refs[-3], refs[-2], refs[-1]
    copies = []
    at = 0
    for ref, (k, start) in zip(parts, slots):
        m = ref.shape[0]
        here = buf.at[pl.ds(at, m)]
        pull = pltpu.make_async_copy(ref, here, sems.at[0, len(copies)])
        push = pltpu.make_async_copy(here, out.at[pl.ds(idx[k] + start, m)], sems.at[1, len(copies)])
        copies.append((pull, push))
        pull.start()
        at += m
    for pull, push in copies:
        pull.wait()
        push.start()
    for _, push in copies:
        push.wait()


def place(idx, parts, slots, out_shape, base=None):
    n = len(parts)
    total = sum(p.shape[0] for p in parts)
    return pl.pallas_call(
        functools.partial(place_kernel, slots=slots),
        in_specs=[pl.BlockSpec(memory_space=pltpu.SMEM)] + [ANY] * (n + (base is not None)),
        out_specs=ANY, out_shape=out_shape, name="place",
        scratch_shapes=[pltpu.VMEM((total,) + parts[0].shape[1:], BF16), pltpu.SemaphoreType.DMA((2, n))],
        input_output_aliases={n + 1: 0} if base is not None else {},
        cost_estimate=pl.CostEstimate(flops=10 ** 9, bytes_accessed=2 * total * 589824, transcendentals=0),
        compiler_params=pltpu.CompilerParams(vmem_limit_bytes=40 * MIB),
    )(idx, *parts, *([base] if base is not None else []))


def column(v, pad=0):
    v = jnp.pad(v, (0, pad)) if pad else v
    return jnp.broadcast_to(v[:, None], (v.shape[0], 128))


def solution(mesh):
    sp = mesh.shape['sp']

    def device_step(images, w_patch, b_patch, pos_embed, ln1_gain, ln1_bias, w_qkv, b_qkv, w_out, b_out, ln2_gain, ln2_bias, w_fc1, b_fc1, w_fc2, b_fc2):
        me = lax.axis_index('sp')
        d = w_patch.shape[3]
        per = images.shape[0] // sp
        planes = jnp.transpose(images, (0, 3, 1, 2))
        x = jnp.arange(512)[:, None]
        o = jnp.arange(512)[None, :]
        px, gx = x % 16, x // 16
        perm = jnp.stack([(o == 128 * (px // 4) + 32 * ((px % 4 + j) % 4) + gx) for j in range(4)]).astype(BF16)
        wp = jnp.transpose(w_patch, (3, 1, 2, 0)).reshape(d, 768)
        pos = pos_embed.T
        bp = column(b_patch)
        wq = jnp.transpose(w_qkv, (1, 2, 3, 0)).reshape(3 * d, d)
        bq = column(b_qkv.reshape(3 * d))
        g1, c1 = column(ln1_gain), column(ln1_bias)
        wo = w_out.reshape(d, d).T
        bo, g2, c2 = column(b_out), column(ln2_gain), column(ln2_bias)
        pad = 4352 - w_fc1.shape[1]
        w1 = w_fc1.T
        b1 = column(b_fc1, pad)
        w2 = flip(w_fc2, 4352, 256)
        b2 = column(b_fc2)

        def swap(a, k):
            return lax.ppermute(a, 'sp', [(i, i ^ k) for i in range(sp)]) if k else a

        peers = [me ^ k for k in range(sp)]
        starts = [sum(CHUNKS[:c]) for c in range(len(CHUNKS))]
        got, where = [], []
        for c, n in enumerate(GROUPS):
            begin = sum(GROUPS[:c])
            idx = jnp.stack([p * per + begin for p in peers]).astype(jnp.int32)
            mine = embed(idx, planes, perm, wp, bp, pos, n)
            got.append([swap(a, k) for k, a in enumerate(mine)])
            where += [(c, i) for i in range(n)]
        owner = jnp.stack([p * per for p in peers]).astype(jnp.int32)
        early, slots, res = [], [], None
        last = len(CHUNKS) - 1
        for c, n in enumerate(CHUNKS):
            group, at = where[starts[c]]
            xs = got[group]
            if c:
                own, _ = lax.optimization_barrier((xs[0], res[0]))
                xs = [own] + xs[1:]
            att = attention(xs, at, n, wq, bq, g1, c1)
            res = mlp(att, xs, at, wo, bo, g2, c2, w1, b1, w2, b2)
            back = [swap(a, k) for k, a in enumerate(res)]
            if c < last:
                early += back
                slots += [(k, starts[c]) for k in range(sp)]
        shape = jax.ShapeDtypeStruct((images.shape[0], 256, d), BF16)
        early, slots = early + back[:1], slots + [(0, starts[last])]
        out = place(owner, early, slots, shape)
        return place(owner, back[1:], [(k, starts[last]) for k in range(1, sp)], shape, out)

    in_specs = (P('dp', 'sp', None, None), P(), P(), P('sp', None)) + (P(),) * 12
    return jax.shard_map(device_step, mesh=mesh, in_specs=in_specs, out_specs=P('dp', 'sp', None), check_vma=False)
```

```python
import functools
import jax
import jax.numpy as jnp
from jax import lax
from jax.experimental import pallas as pl
from jax.experimental.pallas import tpu as pltpu
from jax.sharding import PartitionSpec as P

LN_EPS = 1e-6
GROUPS = (2, 6)
CHUNKS = (2, 3, 2, 1)
MIB = 2 ** 20
F32, BF16 = jnp.float32, jnp.bfloat16


def dot(a, b):
    return jnp.dot(a, b, preferred_element_type=F32)


def widen(col, lanes):
    return jnp.concatenate([col] * (lanes // 128), axis=1)


def embed_kernel(idx_ref, i0, i1, i2, i3, perm_ref, wp_ref, bp_ref, pos_ref, o0, o1, o2, o3, xs):
    imgs = (i0, i1, i2, i3)
    outs = (o0, o1, o2, o3)
    zs = []
    for j in range(4):
        rows = []
        for k in range(4):
            for g in range(2):
                y = (4 * g + j) * 16
                for c in range(3):
                    rows.append(imgs[k][0, c, y:y + 16, :])
        zs.append(dot(jnp.concatenate(rows, axis=0).astype(BF16), perm_ref[j]))
    group = lax.broadcasted_iota(jnp.int32, (48, 128), 1) // 32
    for k in range(4):
        for g in range(2):
            r = (k * 2 + g) * 48
            for v in range(4):
                for u in range(4):
                    acc = zs[0][r:r + 48, 128 * v:128 * v + 128]
                    for j in range(1, 4):
                        acc = jnp.where(group == (u + j) % 4, zs[j][r:r + 48, 128 * v:128 * v + 128], acc)
                    if u:
                        acc = pltpu.roll(acc, 128 - 32 * u, 1)
                    px = 4 * v + u
                    xs[px * 48:px * 48 + 48, k * 256 + g * 128:k * 256 + g * 128 + 128] = acc.astype(BF16)
    step = 384

    def body(m, _):
        ms = pl.multiple_of(m * step, step)
        t = dot(wp_ref[pl.ds(ms, step), :], xs[...])
        t = t + widen(bp_ref[pl.ds(ms, step), :], 1024)
        p = pos_ref[pl.ds(ms, step), :].astype(F32)
        t = (t + jnp.concatenate([p] * 4, axis=1)).astype(BF16)
        for k in range(4):
            outs[k][0, pl.ds(ms, step), :] = t[:, k * 256:(k + 1) * 256]
        return 0

    lax.fori_loop(0, 1152 // step, body, 0)


def embed(idx, planes, perm, wp, bp, pos, n):
    d = wp.shape[0]

    def img(k):
        return pl.BlockSpec((1, 3, 128, 512), lambda i, idx, k=k: (idx[k] + i, 0, 0, 0))

    def whole(a):
        return pl.BlockSpec(a.shape, lambda i, idx: (0,) * a.ndim, pipeline_mode=pl.Buffered(1))

    return pl.pallas_call(
        embed_kernel,
        grid_spec=pltpu.PrefetchScalarGridSpec(
            num_scalar_prefetch=1, grid=(n,),
            in_specs=[img(0), img(1), img(2), img(3), whole(perm), whole(wp), whole(bp), whole(pos)],
            out_specs=[pl.BlockSpec((1, d, 256), lambda i, idx: (i, 0, 0))] * 4,
            scratch_shapes=[pltpu.VMEM((768, 1024), BF16)]),
        out_shape=[jax.ShapeDtypeStruct((n, d, 256), BF16)] * 4,
        name="embed",
        cost_estimate=pl.CostEstimate(flops=2 * n * 1024 * 768 * 1152, bytes_accessed=n * 6 * MIB, transcendentals=0),
        compiler_params=pltpu.CompilerParams(vmem_limit_bytes=56 * MIB),
    )(idx, planes, planes, planes, planes, perm, wp, bp, pos)


def row_mean(x, parts=8):
    rows = x.shape[0] // parts
    sums = [jnp.sum(x[i * rows:(i + 1) * rows].reshape(rows // 8, 8, x.shape[1]), axis=0) for i in range(parts)]
    while len(sums) > 1:
        sums = [p + q for p, q in zip(sums[::2], sums[1::2])]
    return jnp.sum(sums[0], axis=0, keepdims=True) * (1.0 / x.shape[0])


def normed(x, gain, bias):
    cen = x - row_mean(x)
    lanes = x.shape[1]
    return (cen * lax.rsqrt(row_mean(cen * cen) + LN_EPS) * widen(gain, lanes) + widen(bias, lanes)).astype(BF16)


def gelu_of_half(h):
    c = 0.7978845608028654
    return h + h * jnp.tanh(h * (2 * c + (8 * c * 0.044715) * (h * h)))


ANY = pl.BlockSpec(memory_space=pl.ANY)


def attn_kernel(x0, x1, x2, x3, w_hbm, b_hbm, g_ref, c_ref, o_ref, y1, qt, kn, vt, sa, sb, w_ref, b_ref, sems):
    bands = (x0, x1, x2, x3)
    first = pl.program_id(0) == 0
    loads = [pltpu.make_async_copy(b_hbm, b_ref, sems.at[3])]
    for t in range(3):
        rows = pl.ds(t * 1152, 1152)
        loads.append(pltpu.make_async_copy(w_hbm.at[rows, :], w_ref.at[rows, :], sems.at[t]))

    @pl.when(first)
    def _():
        loads[0].start()
        loads[1].start()

    for k in range(4):
        y1[:, k * 256:k * 256 + 256] = normed(bands[k][0].astype(F32), g_ref[...], c_ref[...])
    zero8 = jnp.zeros((8, 1024), F32)
    for t in range(3):
        @pl.when(first)
        def _(t=t):
            if t == 0:
                loads[0].wait()
            loads[t + 1].wait()
            if t < 2:
                loads[t + 2].start()

        def proj(i, _, t=t):
            ms = pl.multiple_of(t * 1152 + i * 576, 576)
            acc = dot(w_ref[pl.ds(ms, 576), :], y1[...]) + widen(b_ref[pl.ds(ms, 576), :], 1024)
            for j in range(8):
                part = jnp.concatenate([acc[j * 72:j * 72 + 72], zero8], axis=0)
                if t == 0:
                    qt[i * 8 + j] = part.astype(BF16)
                elif t == 1:
                    kn[i * 8 + j] = part.T.astype(BF16)
                else:
                    vt[i * 8 + j] = part.astype(BF16)
            return 0
        lax.fori_loop(0, 2, proj, 0)
    scale = 1.4426950408889634 * 72 ** -0.5

    def fold(x, op):
        return op(x.reshape(x.shape[0] // 8, 8, x.shape[1]), axis=0)

    def step(ahead, ahead_buf, h, buf, m):
        top, total, acc = None, None, None
        for c in range(4):
            rows = slice(c * 256, c * 256 + 256)
            s = dot(kn[ahead, rows, :], qt[ahead])
            e = jnp.exp2((buf[rows, :] - m) * scale)
            ahead_buf[rows, :] = s
            t, l, o = fold(s, jnp.max), fold(e, jnp.sum), dot(vt[h, :, rows], e.astype(BF16))
            top = t if top is None else jnp.maximum(top, t)
            total = l if total is None else total + l
            acc = o if acc is None else acc + o
        return jnp.max(top, axis=0, keepdims=True), acc[:72] * (1.0 / jnp.sum(total, axis=0, keepdims=True))

    def tiles(i, m):
        m1, one = step(i * 2 + 1, sb, i * 2, sa, m)
        m2, two = step(jnp.minimum(i * 2 + 2, 15), sa, i * 2 + 1, sb, m1)
        o_ref[0, pl.ds(pl.multiple_of(i * 144, 144), 144), :] = jnp.concatenate([one, two], axis=0).astype(BF16)
        return m2

    s0 = dot(kn[0], qt[0])
    sa[...] = s0
    lax.fori_loop(0, 8, tiles, jnp.max(s0, axis=0, keepdims=True))


def whole1(a):
    return pl.BlockSpec(a.shape, lambda i: (0,) * a.ndim, pipeline_mode=pl.Buffered(1))


def attention(xs, at, n, w, b, g, c):
    d = xs[0].shape[1]
    band = pl.BlockSpec((1, d, 256), lambda i: (i + at, 0, 0))
    return pl.pallas_call(
        attn_kernel, grid=(n,),
        in_specs=[band] * 4 + [ANY, ANY, whole1(g), whole1(c)],
        out_specs=pl.BlockSpec((1, d, 1024), lambda i: (i, 0, 0)),
        out_shape=jax.ShapeDtypeStruct((n, d, 1024), BF16),
        scratch_shapes=[pltpu.VMEM((d, 1024), BF16), pltpu.VMEM((16, 80, 1024), BF16), pltpu.VMEM((16, 1024, 80), BF16), pltpu.VMEM((16, 80, 1024), BF16),
                        pltpu.VMEM((1024, 1024), F32), pltpu.VMEM((1024, 1024), F32),
                        pltpu.VMEM(w.shape, BF16), pltpu.VMEM(b.shape, F32), pltpu.SemaphoreType.DMA((4,))],
        name="attn",
        cost_estimate=pl.CostEstimate(flops=n * 25 * 10 ** 9, bytes_accessed=n * 5 * MIB + 10 * MIB, transcendentals=0),
        compiler_params=pltpu.CompilerParams(vmem_limit_bytes=60 * MIB),
    )(*xs, w, b, g, c)


def mlp_kernel(a_ref, x0, x1, x2, x3, wo_hbm, bo, g_ref, c_ref, w1_hbm, b1_hbm, w2_hbm, b2, o0, o1, o2, o3, r, y2, hh, wo, w1, b1, w2, sems):
    bands = (x0, x1, x2, x3)
    outs = (o0, o1, o2, o3)
    first = pl.program_id(0) == 0
    ff = w1_hbm.shape[0]
    full = w1.shape[0]
    tile = full // 4
    ups = []
    for j in range(4):
        rows = pl.ds(j * tile, min(tile, ff - j * tile))
        ups.append(pltpu.make_async_copy(w1_hbm.at[rows, :], w1.at[rows, :], sems.at[j]))
    load_o = pltpu.make_async_copy(wo_hbm, wo, sems.at[4])
    load_b = pltpu.make_async_copy(b1_hbm, b1, sems.at[5])
    load_2 = pltpu.make_async_copy(w2_hbm, w2, sems.at[6])

    @pl.when(first)
    def _():
        load_o.start()
        w1[ff:full, :] = jnp.zeros((full - ff, w1.shape[1]), BF16)
        load_o.wait()
        load_b.start()
        ups[0].start()
        ups[1].start()

    def proj(i, _):
        ms = pl.multiple_of(i * 576, 576)
        t = dot(wo[pl.ds(ms, 576), :], a_ref[0]) + widen(bo[pl.ds(ms, 576), :], 1024)
        for k in range(4):
            r[pl.ds(ms, 576), k * 256:(k + 1) * 256] = t[:, k * 256:(k + 1) * 256] + bands[k][0, pl.ds(ms, 576), :].astype(F32)
        return 0

    lax.fori_loop(0, 2, proj, 0)

    def norm(i, _):
        ls = pl.multiple_of(i * 256, 256)
        y2[:, pl.ds(ls, 256)] = normed(r[:, pl.ds(ls, 256)], g_ref[...], c_ref[...])
        return 0

    lax.fori_loop(0, 4, norm, 0)

    @pl.when(first)
    def _():
        load_b.wait()

    def up(i, _):
        for j in range(4):
            @pl.when(first & (i == j))
            def _(j=j):
                ups[j].wait()
                if j < 2:
                    ups[j + 2].start()
                elif j == 2:
                    load_2.start()
        ms = pl.multiple_of(i * tile, tile)
        z = dot(w1[pl.ds(ms, tile), :], y2[...]) + widen(b1[pl.ds(ms, tile), :], 1024)
        hh[pl.ds(ms, tile), :] = gelu_of_half(z).astype(BF16)
        return 0

    lax.fori_loop(0, 4, up, 0)

    @pl.when(first)
    def _():
        load_2.wait()

    def down(k, _):
        ls = pl.multiple_of(k * 256, 256)
        t = dot(w2[...], hh[:, pl.ds(ls, 256)]) + widen(b2[...], 256) + r[:, pl.ds(ls, 256)]
        t = t.astype(BF16).T
        for j in range(4):
            @pl.when(k == j)
            def _():
                outs[j][0] = t
        return 0

    lax.fori_loop(0, 4, down, 0)


def mlp(att, xs, at, wo, bo, g, c, w1, b1, w2, b2):
    n, d, _ = att.shape
    f = w2.shape[1]
    band = pl.BlockSpec((1, d, 256), lambda i: (i + at, 0, 0))
    return pl.pallas_call(
        mlp_kernel, grid=(n,),
        in_specs=[pl.BlockSpec((1, d, 1024), lambda i: (i, 0, 0))] + [band] * 4 + [ANY, whole1(bo), whole1(g), whole1(c), ANY, ANY, ANY, whole1(b2)],
        out_specs=[pl.BlockSpec((1, 256, d), lambda i: (i, 0, 0))] * 4,
        out_shape=[jax.ShapeDtypeStruct((n, 256, d), BF16)] * 4,
        scratch_shapes=[pltpu.VMEM((d, 1024), F32), pltpu.VMEM((d, 1024), BF16), pltpu.VMEM((f, 1024), BF16),
                        pltpu.VMEM((d, d), BF16), pltpu.VMEM((f, d), BF16), pltpu.VMEM((f, 128), F32), pltpu.VMEM((d, f), BF16),
                        pltpu.SemaphoreType.DMA((7,))],
        name="mlp",
        cost_estimate=pl.CostEstimate(flops=n * 26 * 10 ** 9, bytes_accessed=n * 8 * MIB + 23 * MIB, transcendentals=0),
        compiler_params=pltpu.CompilerParams(vmem_limit_bytes=63 * MIB),
    )(att, *xs, wo, bo, g, c, w1, b1, w2, b2)


def flip_kernel(w_ref, o_ref, *, rows):
    at = pl.program_id(0) * w_ref.shape[0] + lax.broadcasted_iota(jnp.int32, w_ref.shape, 0)
    o_ref[...] = jnp.where(at < rows, w_ref[...], jnp.zeros_like(w_ref)).T


def flip(w, full, block):
    rows, d = w.shape
    return pl.pallas_call(
        functools.partial(flip_kernel, rows=rows), grid=(full // block,),
        in_specs=[pl.BlockSpec((block, d), lambda i: (i, 0))],
        out_specs=pl.BlockSpec((d, block), lambda i: (0, i)),
        out_shape=jax.ShapeDtypeStruct((d, full), BF16), name="flip",
        cost_estimate=pl.CostEstimate(flops=2 * 10 ** 9, bytes_accessed=20 * MIB, transcendentals=0),
    )(w)


def place_kernel(*refs, slots):
    n = len(slots)
    idx, parts, out, buf, sems = refs[0], refs[1:1 + n], refs[-3], refs[-2], refs[-1]
    copies = []
    at = 0
    for ref, (k, start) in zip(parts, slots):
        m = ref.shape[0]
        here = buf.at[pl.ds(at, m)]
        pull = pltpu.make_async_copy(ref, here, sems.at[0, len(copies)])
        push = pltpu.make_async_copy(here, out.at[pl.ds(idx[k] + start, m)], sems.at[1, len(copies)])
        copies.append((pull, push))
        pull.start()
        at += m
    for pull, push in copies:
        pull.wait()
        push.start()
    for _, push in copies:
        push.wait()


def place(idx, parts, slots, out_shape, base=None):
    n = len(parts)
    total = sum(p.shape[0] for p in parts)
    return pl.pallas_call(
        functools.partial(place_kernel, slots=slots),
        in_specs=[pl.BlockSpec(memory_space=pltpu.SMEM)] + [ANY] * (n + (base is not None)),
        out_specs=ANY, out_shape=out_shape, name="place",
        scratch_shapes=[pltpu.VMEM((total,) + parts[0].shape[1:], BF16), pltpu.SemaphoreType.DMA((2, n))],
        input_output_aliases={n + 1: 0} if base is not None else {},
        cost_estimate=pl.CostEstimate(flops=10 ** 9, bytes_accessed=2 * total * 589824, transcendentals=0),
        compiler_params=pltpu.CompilerParams(vmem_limit_bytes=40 * MIB),
    )(idx, *parts, *([base] if base is not None else []))


def column(v, pad=0):
    v = jnp.pad(v, (0, pad)) if pad else v
    return jnp.broadcast_to(v[:, None], (v.shape[0], 128))


def solution(mesh):
    sp = mesh.shape['sp']

    def device_step(images, w_patch, b_patch, pos_embed, ln1_gain, ln1_bias, w_qkv, b_qkv, w_out, b_out, ln2_gain, ln2_bias, w_fc1, b_fc1, w_fc2, b_fc2):
        me = lax.axis_index('sp')
        d = w_patch.shape[3]
        per = images.shape[0] // sp
        planes = jnp.transpose(images, (0, 3, 1, 2))
        x = jnp.arange(512)[:, None]
        o = jnp.arange(512)[None, :]
        px, gx = x % 16, x // 16
        perm = jnp.stack([(o == 128 * (px // 4) + 32 * ((px % 4 + j) % 4) + gx) for j in range(4)]).astype(BF16)
        wp = jnp.transpose(w_patch, (3, 1, 2, 0)).reshape(d, 768)
        pos = pos_embed.T
        bp = column(b_patch)
        wq = jnp.transpose(w_qkv, (1, 2, 3, 0)).reshape(3 * d, d)
        bq = column(b_qkv.reshape(3 * d))
        g1, c1 = column(ln1_gain), column(ln1_bias)
        wo = w_out.reshape(d, d).T
        bo, g2, c2 = column(b_out), column(ln2_gain * 0.5), column(ln2_bias * 0.5)
        pad = 4352 - w_fc1.shape[1]
        w1 = w_fc1.T
        b1 = column(b_fc1 * 0.5, pad)
        w2 = flip(w_fc2, 4352, 256)
        b2 = column(b_fc2)

        def swap(a, k):
            return lax.ppermute(a, 'sp', [(i, i ^ k) for i in range(sp)]) if k else a

        peers = [me ^ k for k in range(sp)]
        starts = [sum(CHUNKS[:c]) for c in range(len(CHUNKS))]
        got, where = [], []
        for c, n in enumerate(GROUPS):
            begin = sum(GROUPS[:c])
            idx = jnp.stack([p * per + begin for p in peers]).astype(jnp.int32)
            mine = embed(idx, planes, perm, wp, bp, pos, n)
            got.append([swap(a, k) for k, a in enumerate(mine)])
            where += [(c, i) for i in range(n)]
        owner = jnp.stack([p * per for p in peers]).astype(jnp.int32)
        early, slots, res = [], [], None
        last = len(CHUNKS) - 1
        for c, n in enumerate(CHUNKS):
            group, at = where[starts[c]]
            xs = got[group]
            if c:
                own, _ = lax.optimization_barrier((xs[0], res[0]))
                xs = [own] + xs[1:]
            att = attention(xs, at, n, wq, bq, g1, c1)
            res = mlp(att, xs, at, wo, bo, g2, c2, w1, b1, w2, b2)
            back = [swap(a, k) for k, a in enumerate(res)]
            if c < last:
                early += back
                slots += [(k, starts[c]) for k in range(sp)]
        shape = jax.ShapeDtypeStruct((images.shape[0], 256, d), BF16)
        early, slots = early + back[:1], slots + [(0, starts[last])]
        out = place(owner, early, slots, shape)
        return place(owner, back[1:], [(k, starts[last]) for k in range(1, sp)], shape, out)

    in_specs = (P('dp', 'sp', None, None), P(), P(), P('sp', None)) + (P(),) * 12
    return jax.shard_map(device_step, mesh=mesh, in_specs=in_specs, out_specs=P('dp', 'sp', None), check_vma=False)
```

```python
import functools
import jax
import jax.numpy as jnp
from jax import lax
from jax.experimental import pallas as pl
from jax.experimental.pallas import tpu as pltpu
from jax.sharding import PartitionSpec as P


LN_EPS = 1e-6
GROUPS = (2, 6)
CHUNKS = (2, 3, 2, 1)
DOWN = 512
MIB = 2 ** 20
F32, BF16 = jnp.float32, jnp.bfloat16


def dot(a, b):
    return jnp.dot(a, b, preferred_element_type=F32)


def widen(col, lanes):
    return jnp.concatenate([col] * (lanes // 128), axis=1)


def embed_kernel(idx_ref, i0, i1, i2, i3, perm_ref, wp_ref, bp_ref, pos_ref, o0, o1, o2, o3, xs):
    imgs = (i0, i1, i2, i3)
    outs = (o0, o1, o2, o3)
    zs = []
    for j in range(4):
        rows = []
        for k in range(4):
            for g in range(2):
                y = (4 * g + j) * 16
                for c in range(3):
                    rows.append(imgs[k][0, c, y:y + 16, :])
        zs.append(dot(jnp.concatenate(rows, axis=0).astype(BF16), perm_ref[j]))
    group = lax.broadcasted_iota(jnp.int32, (48, 128), 1) // 32
    for k in range(4):
        for g in range(2):
            r = (k * 2 + g) * 48
            for v in range(4):
                for u in range(4):
                    acc = zs[0][r:r + 48, 128 * v:128 * v + 128]
                    for j in range(1, 4):
                        acc = jnp.where(group == (u + j) % 4, zs[j][r:r + 48, 128 * v:128 * v + 128], acc)
                    if u:
                        acc = pltpu.roll(acc, 128 - 32 * u, 1)
                    px = 4 * v + u
                    xs[px * 48:px * 48 + 48, k * 256 + g * 128:k * 256 + g * 128 + 128] = acc.astype(BF16)
    step = 384

    def body(m, _):
        ms = pl.multiple_of(m * step, step)
        t = dot(wp_ref[pl.ds(ms, step), :], xs[...])
        t = t + widen(bp_ref[pl.ds(ms, step), :], 1024)
        p = pos_ref[pl.ds(ms, step), :].astype(F32)
        t = (t + jnp.concatenate([p] * 4, axis=1)).astype(BF16)
        for k in range(4):
            outs[k][0, pl.ds(ms, step), :] = t[:, k * 256:(k + 1) * 256]
        return 0

    lax.fori_loop(0, 1152 // step, body, 0)


def embed(idx, planes, perm, wp, bp, pos, n):
    d = wp.shape[0]

    def img(k):
        return pl.BlockSpec((1, 3, 128, 512), lambda i, idx, k=k: (idx[k] + i, 0, 0, 0))

    def whole(a):
        return pl.BlockSpec(a.shape, lambda i, idx: (0,) * a.ndim, pipeline_mode=pl.Buffered(1))

    return pl.pallas_call(
        embed_kernel,
        grid_spec=pltpu.PrefetchScalarGridSpec(
            num_scalar_prefetch=1, grid=(n,),
            in_specs=[img(0), img(1), img(2), img(3), whole(perm), whole(wp), whole(bp), whole(pos)],
            out_specs=[pl.BlockSpec((1, d, 256), lambda i, idx: (i, 0, 0))] * 4,
            scratch_shapes=[pltpu.VMEM((768, 1024), BF16)]),
        out_shape=[jax.ShapeDtypeStruct((n, d, 256), BF16)] * 4,
        name="embed",
        cost_estimate=pl.CostEstimate(flops=2 * n * 1024 * 768 * 1152, bytes_accessed=n * 6 * MIB, transcendentals=0),
        compiler_params=pltpu.CompilerParams(vmem_limit_bytes=56 * MIB),
    )(idx, planes, planes, planes, planes, perm, wp, bp, pos)


def row_mean(x, parts=8):
    rows = x.shape[0] // parts
    sums = [jnp.sum(x[i * rows:(i + 1) * rows].reshape(rows // 8, 8, x.shape[1]), axis=0) for i in range(parts)]
    while len(sums) > 1:
        sums = [p + q for p, q in zip(sums[::2], sums[1::2])]
    return jnp.sum(sums[0], axis=0, keepdims=True) * (1.0 / x.shape[0])


def normed(x, gain, bias):
    cen = x - row_mean(x)
    lanes = x.shape[1]
    return (cen * lax.rsqrt(row_mean(cen * cen) + LN_EPS) * widen(gain, lanes) + widen(bias, lanes)).astype(BF16)


def gelu_of_half(h):
    c = 0.7978845608028654
    return h + h * jnp.tanh(h * (2 * c + (8 * c * 0.044715) * (h * h)))


ANY = pl.BlockSpec(memory_space=pl.ANY)


def attn_kernel(x0, x1, x2, x3, w_hbm, b_hbm, g_ref, c_ref, o_ref, y1, qt, kn, vt, sa, sb, w_ref, b_ref, sems):
    bands = (x0, x1, x2, x3)
    first = pl.program_id(0) == 0
    loads = [pltpu.make_async_copy(b_hbm, b_ref, sems.at[3])]
    for t in range(3):
        rows = pl.ds(t * 1152, 1152)
        loads.append(pltpu.make_async_copy(w_hbm.at[rows, :], w_ref.at[rows, :], sems.at[t]))

    @pl.when(first)
    def _():
        loads[0].start()
        loads[1].start()

    for k in range(4):
        y1[:, k * 256:k * 256 + 256] = normed(bands[k][0].astype(F32), g_ref[...], c_ref[...])
    zero8 = jnp.zeros((8, 1024), F32)
    for t in range(3):
        @pl.when(first)
        def _(t=t):
            if t == 0:
                loads[0].wait()
            loads[t + 1].wait()
            if t < 2:
                loads[t + 2].start()

        def proj(i, _, t=t):
            ms = pl.multiple_of(t * 1152 + i * 576, 576)
            acc = dot(w_ref[pl.ds(ms, 576), :], y1[...]) + widen(b_ref[pl.ds(ms, 576), :], 1024)
            for j in range(8):
                part = jnp.concatenate([acc[j * 72:j * 72 + 72], zero8], axis=0)
                if t == 0:
                    qt[i * 8 + j] = part.astype(BF16)
                elif t == 1:
                    kn[i * 8 + j] = part.T.astype(BF16)
                else:
                    vt[i * 8 + j] = part.astype(BF16)
            return 0

        lax.fori_loop(0, 2, proj, 0)
    scale = 1.4426950408889634 * 72 ** -0.5

    def fold(x, op):
        return op(x.reshape(x.shape[0] // 8, 8, x.shape[1]), axis=0)

    def step(ahead, ahead_buf, h, buf, m):
        top, total, acc = None, None, None
        for c in range(4):
            rows = slice(c * 256, c * 256 + 256)
            s = dot(kn[ahead, rows, :], qt[ahead])
            e = jnp.exp2((buf[rows, :] - m) * scale)
            ahead_buf[rows, :] = s
            t, l, o = fold(s, jnp.max), fold(e, jnp.sum), dot(vt[h, :, rows], e.astype(BF16))
            top = t if top is None else jnp.maximum(top, t)
            total = l if total is None else total + l
            acc = o if acc is None else acc + o
        return jnp.max(top, axis=0, keepdims=True), acc[:72] * (1.0 / jnp.sum(total, axis=0, keepdims=True))

    def tiles(i, m):
        m1, one = step(i * 2 + 1, sb, i * 2, sa, m)
        m2, two = step(jnp.minimum(i * 2 + 2, 15), sa, i * 2 + 1, sb, m1)
        o_ref[0, pl.ds(pl.multiple_of(i * 144, 144), 144), :] = jnp.concatenate([one, two], axis=0).astype(BF16)
        return m2

    s0 = dot(kn[0], qt[0])
    sa[...] = s0
    lax.fori_loop(0, 8, tiles, jnp.max(s0, axis=0, keepdims=True))


def whole1(a):
    return pl.BlockSpec(a.shape, lambda i: (0,) * a.ndim, pipeline_mode=pl.Buffered(1))


def attention(xs, at, n, w, b, g, c):
    d = xs[0].shape[1]
    band = pl.BlockSpec((1, d, 256), lambda i: (i + at, 0, 0))
    return pl.pallas_call(
        attn_kernel, grid=(n,),
        in_specs=[band] * 4 + [ANY, ANY, whole1(g), whole1(c)],
        out_specs=pl.BlockSpec((1, d, 1024), lambda i: (i, 0, 0)),
        out_shape=jax.ShapeDtypeStruct((n, d, 1024), BF16),
        scratch_shapes=[pltpu.VMEM((d, 1024), BF16), pltpu.VMEM((16, 80, 1024), BF16), pltpu.VMEM((16, 1024, 80), BF16), pltpu.VMEM((16, 80, 1024), BF16),
                        pltpu.VMEM((1024, 1024), F32), pltpu.VMEM((1024, 1024), F32),
                        pltpu.VMEM(w.shape, BF16), pltpu.VMEM(b.shape, F32), pltpu.SemaphoreType.DMA((4,))],
        name="attn",
        cost_estimate=pl.CostEstimate(flops=n * 25 * 10 ** 9, bytes_accessed=n * 5 * MIB + 10 * MIB, transcendentals=0),
        compiler_params=pltpu.CompilerParams(vmem_limit_bytes=60 * MIB),
    )(*xs, w, b, g, c)


def place_moves(idx, parts, slots, out, buf, sems):
    moves = []
    at = 0
    for ref, (k, start) in zip(parts, slots):
        m = ref.shape[0]
        here = buf.at[pl.ds(at, m)]
        moves.append((pltpu.make_async_copy(ref, here, sems.at[0, len(moves)]),
                      pltpu.make_async_copy(here, out.at[pl.ds(idx[k] + start, m)], sems.at[1, len(moves)])))
        at += m
    return moves


def mlp_kernel(*refs, nb, slots):
    a_ref, bands = refs[0], refs[1:1 + nb]
    wo_hbm, bo, g_ref, c_ref, w1_hbm, b1_hbm, w2_hbm, b2 = refs[1 + nb:9 + nb]
    refs = refs[9 + nb:]
    moves = []
    if slots:
        idx, parts, out, buf, move_sems = refs[0], refs[1:1 + len(slots)], refs[1 + len(slots) + nb], refs[-2], refs[-1]
        moves = place_moves(idx, parts, slots, out, buf, move_sems)
        refs = refs[1 + len(slots):1 + len(slots) + nb] + refs[2 + len(slots) + nb:-2]
    outs = refs[:nb]
    r, y2, hh, wo, w1, b1, w2, sems = refs[nb:]
    lanes = nb * 256
    first = pl.program_id(0) == 0
    ff = w1_hbm.shape[0]
    full = w1.shape[0]
    tile = full // 4
    ups = []
    for j in range(4):
        rows = pl.ds(j * tile, min(tile, ff - j * tile))
        ups.append(pltpu.make_async_copy(w1_hbm.at[rows, :], w1.at[rows, :], sems.at[j]))
    load_o = pltpu.make_async_copy(wo_hbm, wo, sems.at[4])
    load_b = pltpu.make_async_copy(b1_hbm, b1, sems.at[5])
    load_2 = pltpu.make_async_copy(w2_hbm, w2, sems.at[6])

    @pl.when(first)
    def _():
        load_o.start()
        w1[ff:full, :] = jnp.zeros((full - ff, w1.shape[1]), BF16)
        load_o.wait()
        load_b.start()
        ups[0].start()
        ups[1].start()

    for pull, _ in moves:
        pull.start()

    def proj(i, _):
        ms = pl.multiple_of(i * 576, 576)
        t = dot(wo[pl.ds(ms, 576), :], a_ref[0]) + widen(bo[pl.ds(ms, 576), :], lanes)
        for k in range(nb):
            r[pl.ds(ms, 576), k * 256:(k + 1) * 256] = t[:, k * 256:(k + 1) * 256] + bands[k][0, pl.ds(ms, 576), :].astype(F32)
        return 0

    lax.fori_loop(0, 2, proj, 0)

    def norm(i, _):
        ls = pl.multiple_of(i * 256, 256)
        y2[:, pl.ds(ls, 256)] = normed(r[:, pl.ds(ls, 256)], g_ref[...], c_ref[...])
        return 0

    lax.fori_loop(0, nb, norm, 0)

    @pl.when(first)
    def _():
        load_b.wait()

    def up(i, _):
        for j in range(4):
            @pl.when(first & (i == j))
            def _(j=j):
                ups[j].wait()
                if j < 2:
                    ups[j + 2].start()
                elif j == 2:
                    load_2.start()
        ms = pl.multiple_of(i * tile, tile)
        z = dot(w1[pl.ds(ms, tile), :], y2[...]) + widen(b1[pl.ds(ms, tile), :], lanes)
        hh[pl.ds(ms, tile), :] = gelu_of_half(z).astype(BF16)
        return 0

    lax.fori_loop(0, 4, up, 0)
    for pull, push in moves:
        pull.wait()
        push.start()

    @pl.when(first)
    def _():
        load_2.wait()

    def down(i, _):
        ls = pl.multiple_of(i * DOWN, DOWN)
        t = dot(w2[...], hh[:, pl.ds(ls, DOWN)]) + widen(b2[...], DOWN) + r[:, pl.ds(ls, DOWN)]
        t = t.astype(BF16).T
        step = DOWN // 256
        for j in range(nb // step):
            @pl.when(i == j)
            def _():
                for q in range(step):
                    outs[j * step + q][0] = t[q * 256:(q + 1) * 256]
        return 0

    lax.fori_loop(0, lanes // DOWN, down, 0)
    for _, push in moves:
        push.wait()


def mlp(att, xs, at, ks, wo, bo, g, c, w1, b1, w2, b2, idx=None, parts=(), slots=(), shape=None):
    n, d, _ = att.shape
    f = w2.shape[1]
    nb = len(ks)
    lanes = nb * 256
    half = ks[0] // nb
    band = pl.BlockSpec((1, d, 256), lambda i: (i + at, 0, 0))
    extra = [idx, *parts] if parts else []
    total = sum(p.shape[0] for p in parts)
    room = [pltpu.VMEM((total, 256, d), BF16), pltpu.SemaphoreType.DMA((2, len(parts)))] if parts else []
    return pl.pallas_call(
        functools.partial(mlp_kernel, nb=nb, slots=slots), grid=(n,),
        in_specs=[pl.BlockSpec((1, d, lanes), lambda i: (i, 0, half))] + [band] * nb + [ANY, whole1(bo), whole1(g), whole1(c), ANY, ANY, ANY, whole1(b2)]
        + ([pl.BlockSpec(memory_space=pltpu.SMEM)] + [ANY] * len(parts) if parts else []),
        out_specs=[pl.BlockSpec((1, 256, d), lambda i: (i, 0, 0))] * nb + ([ANY] if parts else []),
        out_shape=[jax.ShapeDtypeStruct((n, 256, d), BF16)] * nb + ([shape] if parts else []),
        scratch_shapes=[pltpu.VMEM((d, lanes), F32), pltpu.VMEM((d, lanes), BF16), pltpu.VMEM((f, lanes), BF16),
                        pltpu.VMEM((d, d), BF16), pltpu.VMEM((f, d), BF16), pltpu.VMEM((f, 128), F32), pltpu.VMEM((d, f), BF16),
                        pltpu.SemaphoreType.DMA((7,))] + room,
        name="mlp",
        cost_estimate=pl.CostEstimate(flops=n * nb * 6 * 10 ** 9, bytes_accessed=n * 8 * MIB + 23 * MIB, transcendentals=0),
        compiler_params=pltpu.CompilerParams(vmem_limit_bytes=63 * MIB),
    )(att, *[xs[k] for k in ks], wo, bo, g, c, w1, b1, w2, b2, *extra)


def flip_kernel(w_ref, o_ref, *, rows):
    at = pl.program_id(0) * w_ref.shape[0] + lax.broadcasted_iota(jnp.int32, w_ref.shape, 0)
    o_ref[...] = jnp.where(at < rows, w_ref[...], jnp.zeros_like(w_ref)).T


def flip(w, full, block):
    rows, d = w.shape
    return pl.pallas_call(
        functools.partial(flip_kernel, rows=rows), grid=(full // block,),
        in_specs=[pl.BlockSpec((block, d), lambda i: (i, 0))],
        out_specs=pl.BlockSpec((d, block), lambda i: (0, i)),
        out_shape=jax.ShapeDtypeStruct((d, full), BF16), name="flip",
        cost_estimate=pl.CostEstimate(flops=2 * 10 ** 9, bytes_accessed=20 * MIB, transcendentals=0),
    )(w)


def place_kernel(*refs, slots):
    n = len(slots)
    moves = place_moves(refs[0], refs[1:1 + n], slots, refs[-3], refs[-2], refs[-1])
    for pull, _ in moves:
        pull.start()
    for pull, push in moves:
        pull.wait()
        push.start()
    for _, push in moves:
        push.wait()


def place(idx, parts, slots, out_shape, base=None):
    n = len(parts)
    total = sum(p.shape[0] for p in parts)
    return pl.pallas_call(
        functools.partial(place_kernel, slots=slots),
        in_specs=[pl.BlockSpec(memory_space=pltpu.SMEM)] + [ANY] * (n + (base is not None)),
        out_specs=ANY, out_shape=out_shape, name="place",
        scratch_shapes=[pltpu.VMEM((total,) + parts[0].shape[1:], BF16), pltpu.SemaphoreType.DMA((2, n))],
        input_output_aliases={n + 1: 0} if base is not None else {},
        cost_estimate=pl.CostEstimate(flops=10 ** 9, bytes_accessed=2 * total * 589824, transcendentals=0),
        compiler_params=pltpu.CompilerParams(vmem_limit_bytes=40 * MIB),
    )(idx, *parts, *([base] if base is not None else []))


def column(v, pad=0):
    v = jnp.pad(v, (0, pad)) if pad else v
    return jnp.broadcast_to(v[:, None], (v.shape[0], 128))


def solution(mesh):
    sp = mesh.shape['sp']

    def device_step(images, w_patch, b_patch, pos_embed, ln1_gain, ln1_bias, w_qkv, b_qkv, w_out, b_out, ln2_gain, ln2_bias, w_fc1, b_fc1, w_fc2, b_fc2):
        me = lax.axis_index('sp')
        d = w_patch.shape[3]
        per = images.shape[0] // sp
        planes = jnp.transpose(images, (0, 3, 1, 2))
        x = jnp.arange(512)[:, None]
        o = jnp.arange(512)[None, :]
        px, gx = x % 16, x // 16
        perm = jnp.stack([(o == 128 * (px // 4) + 32 * ((px % 4 + j) % 4) + gx) for j in range(4)]).astype(BF16)
        wp = jnp.transpose(w_patch, (3, 1, 2, 0)).reshape(d, 768)
        pos = pos_embed.T
        bp = column(b_patch)
        wq = jnp.transpose(w_qkv, (1, 2, 3, 0)).reshape(3 * d, d)
        bq = column(b_qkv.reshape(3 * d))
        g1, c1 = column(ln1_gain), column(ln1_bias)
        wo = w_out.reshape(d, d).T
        bo, g2, c2 = column(b_out), column(ln2_gain * 0.5), column(ln2_bias * 0.5)
        pad = 4352 - w_fc1.shape[1]
        w1 = w_fc1.T
        b1 = column(b_fc1 * 0.5, pad)
        w2 = flip(w_fc2, 4352, 256)
        b2 = column(b_fc2)

        def swap(a, k):
            return lax.ppermute(a, 'sp', [(i, i ^ k) for i in range(sp)]) if k else a

        peers = [me ^ k for k in range(sp)]
        starts = [sum(CHUNKS[:c]) for c in range(len(CHUNKS))]
        got, where = [], []
        for c, n in enumerate(GROUPS):
            begin = sum(GROUPS[:c])
            idx = jnp.stack([p * per + begin for p in peers]).astype(jnp.int32)
            mine = embed(idx, planes, perm, wp, bp, pos, n)
            got.append([swap(a, k) for k, a in enumerate(mine)])
            where += [(c, i) for i in range(n)]
        owner = jnp.stack([p * per for p in peers]).astype(jnp.int32)
        early, slots, res = [], [], None
        shape = jax.ShapeDtypeStruct((images.shape[0], 256, d), BF16)
        last = len(CHUNKS) - 1
        for c, n in enumerate(CHUNKS):
            group, at = where[starts[c]]
            xs = got[group]
            if c:
                own, _ = lax.optimization_barrier((xs[0], res[0]))
                xs = [own] + xs[1:]
            att = attention(xs, at, n, wq, bq, g1, c1)
            if c < last:
                res = mlp(att, xs, at, (0, 1, 2, 3), wo, bo, g2, c2, w1, b1, w2, b2)
                back = [swap(a, k) for k, a in enumerate(res)]
                early += back
                slots += [(k, starts[c]) for k in range(sp)]
            else:
                far = mlp(att, xs, at, (2, 3), wo, bo, g2, c2, w1, b1, w2, b2)
                own, _ = lax.optimization_barrier((xs[0], far[0]))
                near = mlp(att, [own] + xs[1:], at, (0, 1), wo, bo, g2, c2, w1, b1, w2, b2, owner, early, slots, shape)
                back = [near[0], swap(near[1], 1), swap(far[0], 2), swap(far[1], 3)]
        return place(owner, back, [(k, starts[last]) for k in range(sp)], shape, near[2])

    in_specs = (P('dp', 'sp', None, None), P(), P(), P('sp', None)) + (P(),) * 12
    return jax.shard_map(device_step, mesh=mesh, in_specs=in_specs, out_specs=P('dp', 'sp', None), check_vma=False)
```

```python
import functools
import jax
import jax.numpy as jnp
from jax import lax
from jax.experimental import pallas as pl
from jax.experimental.pallas import tpu as pltpu
from jax.sharding import PartitionSpec as P


LN_EPS = 1e-6
GROUPS = (2, 6)
CHUNKS = (2, 3, 2, 1)
DOWN = 512
MIB = 2 ** 20
F32, BF16 = jnp.float32, jnp.bfloat16


def dot(a, b):
    return jnp.dot(a, b, preferred_element_type=F32)


def widen(col, lanes):
    return jnp.concatenate([col] * (lanes // 128), axis=1)


def embed_kernel(idx_ref, i0, i1, i2, i3, perm_ref, wp_ref, bp_ref, pos_ref, o0, o1, o2, o3, xs):
    imgs = (i0, i1, i2, i3)
    outs = (o0, o1, o2, o3)
    zs = []
    for j in range(4):
        rows = []
        for k in range(4):
            for g in range(2):
                y = (4 * g + j) * 16
                for c in range(3):
                    rows.append(imgs[k][0, c, y:y + 16, :])
        zs.append(dot(jnp.concatenate(rows, axis=0).astype(BF16), perm_ref[j]))
    group = lax.broadcasted_iota(jnp.int32, (48, 128), 1) // 32
    for k in range(4):
        for g in range(2):
            r = (k * 2 + g) * 48
            for v in range(4):
                for u in range(4):
                    acc = zs[0][r:r + 48, 128 * v:128 * v + 128]
                    for j in range(1, 4):
                        acc = jnp.where(group == (u + j) % 4, zs[j][r:r + 48, 128 * v:128 * v + 128], acc)
                    if u:
                        acc = pltpu.roll(acc, 128 - 32 * u, 1)
                    px = 4 * v + u
                    xs[px * 48:px * 48 + 48, k * 256 + g * 128:k * 256 + g * 128 + 128] = acc.astype(BF16)
    step = 384

    def body(m, _):
        ms = pl.multiple_of(m * step, step)
        t = dot(wp_ref[pl.ds(ms, step), :], xs[...])
        t = t + widen(bp_ref[pl.ds(ms, step), :], 1024)
        p = pos_ref[pl.ds(ms, step), :].astype(F32)
        t = (t + jnp.concatenate([p] * 4, axis=1)).astype(BF16)
        for k in range(4):
            outs[k][0, pl.ds(ms, step), :] = t[:, k * 256:(k + 1) * 256]
        return 0

    lax.fori_loop(0, 1152 // step, body, 0)


def embed(idx, planes, perm, wp, bp, pos, n):
    d = wp.shape[0]

    def img(k):
        return pl.BlockSpec((1, 3, 128, 512), lambda i, idx, k=k: (idx[k] + i, 0, 0, 0))

    def whole(a):
        return pl.BlockSpec(a.shape, lambda i, idx: (0,) * a.ndim, pipeline_mode=pl.Buffered(1))

    return pl.pallas_call(
        embed_kernel,
        grid_spec=pltpu.PrefetchScalarGridSpec(
            num_scalar_prefetch=1, grid=(n,),
            in_specs=[img(0), img(1), img(2), img(3), whole(perm), whole(wp), whole(bp), whole(pos)],
            out_specs=[pl.BlockSpec((1, d, 256), lambda i, idx: (i, 0, 0))] * 4,
            scratch_shapes=[pltpu.VMEM((768, 1024), BF16)]),
        out_shape=[jax.ShapeDtypeStruct((n, d, 256), BF16)] * 4,
        name="embed",
        cost_estimate=pl.CostEstimate(flops=2 * n * 1024 * 768 * 1152, bytes_accessed=n * 6 * MIB, transcendentals=0),
        compiler_params=pltpu.CompilerParams(vmem_limit_bytes=56 * MIB),
    )(idx, planes, planes, planes, planes, perm, wp, bp, pos)


def row_mean(x, parts=8):
    rows = x.shape[0] // parts
    sums = [jnp.sum(x[i * rows:(i + 1) * rows].reshape(rows // 8, 8, x.shape[1]), axis=0) for i in range(parts)]
    while len(sums) > 1:
        sums = [p + q for p, q in zip(sums[::2], sums[1::2])]
    return jnp.sum(sums[0], axis=0, keepdims=True) * (1.0 / x.shape[0])


def normed(x, gain, bias):
    cen = x - row_mean(x)
    lanes = x.shape[1]
    return (cen * lax.rsqrt(row_mean(cen * cen) + LN_EPS) * widen(gain, lanes) + widen(bias, lanes)).astype(BF16)


def gelu_of_half(h):
    c = 0.7978845608028654
    return h + h * jnp.tanh(h * (2 * c + (8 * c * 0.044715) * (h * h)))


ANY = pl.BlockSpec(memory_space=pl.ANY)


def attn_kernel(x0, x1, x2, x3, w_hbm, b_hbm, g_ref, c_ref, o_ref, y1, qt, kn, vt, sa, sb, w_ref, b_ref, sems):
    bands = (x0, x1, x2, x3)
    first = pl.program_id(0) == 0
    loads = [pltpu.make_async_copy(b_hbm, b_ref, sems.at[3])]
    for t in range(3):
        rows = pl.ds(t * 1152, 1152)
        loads.append(pltpu.make_async_copy(w_hbm.at[rows, :], w_ref.at[rows, :], sems.at[t]))

    @pl.when(first)
    def _():
        loads[0].start()
        loads[1].start()

    for k in range(4):
        y1[:, k * 256:k * 256 + 256] = normed(bands[k][0].astype(F32), g_ref[...], c_ref[...])
    zero8 = jnp.zeros((8, 1024), F32)
    for t in range(3):
        @pl.when(first)
        def _(t=t):
            if t == 0:
                loads[0].wait()
            loads[t + 1].wait()
            if t < 2:
                loads[t + 2].start()

        def proj(t=t):
            rows = slice(t * 1152, t * 1152 + 1152)
            acc = dot(w_ref[rows, :], y1[...]) + widen(b_ref[rows, :], 1024)
            for j in range(16):
                part = jnp.concatenate([acc[j * 72:j * 72 + 72], zero8], axis=0)
                if t == 0:
                    qt[j] = part.astype(BF16)
                elif t == 1:
                    kn[j] = part.T.astype(BF16)
                else:
                    vt[j] = part.astype(BF16)
            return 0

        proj()
    scale = 1.4426950408889634 * 72 ** -0.5

    def fold(x, op):
        return op(x.reshape(x.shape[0] // 8, 8, x.shape[1]), axis=0)

    def step(ahead, ahead_buf, h, buf, m):
        top, total, acc = None, None, None
        for c in range(4):
            rows = slice(c * 256, c * 256 + 256)
            s = dot(kn[ahead, rows, :], qt[ahead])
            e = jnp.exp2((buf[rows, :] - m) * scale)
            ahead_buf[rows, :] = s
            t, l, o = fold(s, jnp.max), fold(e, jnp.sum), dot(vt[h, :, rows], e.astype(BF16))
            top = t if top is None else jnp.maximum(top, t)
            total = l if total is None else total + l
            acc = o if acc is None else acc + o
        return jnp.max(top, axis=0, keepdims=True), acc[:72] * (1.0 / jnp.sum(total, axis=0, keepdims=True))

    def tiles(i, m):
        m1, one = step(i * 2 + 1, sb, i * 2, sa, m)
        m2, two = step(jnp.minimum(i * 2 + 2, 15), sa, i * 2 + 1, sb, m1)
        o_ref[0, pl.ds(pl.multiple_of(i * 144, 144), 144), :] = jnp.concatenate([one, two], axis=0).astype(BF16)
        return m2

    s0 = dot(kn[0], qt[0])
    sa[...] = s0
    lax.fori_loop(0, 8, tiles, jnp.max(s0, axis=0, keepdims=True))


def whole1(a):
    return pl.BlockSpec(a.shape, lambda i: (0,) * a.ndim, pipeline_mode=pl.Buffered(1))


def attention(xs, at, n, w, b, g, c):
    d = xs[0].shape[1]
    band = pl.BlockSpec((1, d, 256), lambda i: (i + at, 0, 0))
    return pl.pallas_call(
        attn_kernel, grid=(n,),
        in_specs=[band] * 4 + [ANY, ANY, whole1(g), whole1(c)],
        out_specs=pl.BlockSpec((1, d, 1024), lambda i: (i, 0, 0)),
        out_shape=jax.ShapeDtypeStruct((n, d, 1024), BF16),
        scratch_shapes=[pltpu.VMEM((d, 1024), BF16), pltpu.VMEM((16, 80, 1024), BF16), pltpu.VMEM((16, 1024, 80), BF16), pltpu.VMEM((16, 80, 1024), BF16),
                        pltpu.VMEM((1024, 1024), F32), pltpu.VMEM((1024, 1024), F32),
                        pltpu.VMEM(w.shape, BF16), pltpu.VMEM(b.shape, F32), pltpu.SemaphoreType.DMA((4,))],
        name="attn",
        cost_estimate=pl.CostEstimate(flops=n * 25 * 10 ** 9, bytes_accessed=n * 5 * MIB + 10 * MIB, transcendentals=0),
        compiler_params=pltpu.CompilerParams(vmem_limit_bytes=60 * MIB),
    )(*xs, w, b, g, c)


def place_moves(idx, parts, slots, out, buf, sems):
    moves = []
    at = 0
    for ref, (k, start) in zip(parts, slots):
        m = ref.shape[0]
        here = buf.at[pl.ds(at, m)]
        moves.append((pltpu.make_async_copy(ref, here, sems.at[0, len(moves)]),
                      pltpu.make_async_copy(here, out.at[pl.ds(idx[k] + start, m)], sems.at[1, len(moves)])))
        at += m
    return moves


def mlp_kernel(*refs, nb, slots):
    a_ref, bands = refs[0], refs[1:1 + nb]
    wo_hbm, bo, g_ref, c_ref, w1_hbm, b1_hbm, w2_hbm, b2 = refs[1 + nb:9 + nb]
    refs = refs[9 + nb:]
    moves = []
    if slots:
        idx, parts, out, buf, move_sems = refs[0], refs[1:1 + len(slots)], refs[1 + len(slots) + nb], refs[-2], refs[-1]
        moves = place_moves(idx, parts, slots, out, buf, move_sems)
        refs = refs[1 + len(slots):1 + len(slots) + nb] + refs[2 + len(slots) + nb:-2]
    outs = refs[:nb]
    r, y2, hh, wo, w1, b1, w2, sems = refs[nb:]
    lanes = nb * 256
    first = pl.program_id(0) == 0
    ff = w1_hbm.shape[0]
    full = w1.shape[0]
    tile = full // 4
    ups = []
    for j in range(4):
        rows = pl.ds(j * tile, min(tile, ff - j * tile))
        ups.append(pltpu.make_async_copy(w1_hbm.at[rows, :], w1.at[rows, :], sems.at[j]))
    load_o = pltpu.make_async_copy(wo_hbm, wo, sems.at[4])
    load_b = pltpu.make_async_copy(b1_hbm, b1, sems.at[5])
    load_2 = pltpu.make_async_copy(w2_hbm, w2, sems.at[6])

    @pl.when(first)
    def _():
        load_o.start()
        w1[ff:full, :] = jnp.zeros((full - ff, w1.shape[1]), BF16)
        load_o.wait()
        load_b.start()
        ups[0].start()
        ups[1].start()

    for pull, _ in moves:
        pull.start()

    def proj(i, _):
        ms = pl.multiple_of(i * 576, 576)
        t = dot(wo[pl.ds(ms, 576), :], a_ref[0]) + widen(bo[pl.ds(ms, 576), :], lanes)
        for k in range(nb):
            r[pl.ds(ms, 576), k * 256:(k + 1) * 256] = t[:, k * 256:(k + 1) * 256] + bands[k][0, pl.ds(ms, 576), :].astype(F32)
        return 0

    lax.fori_loop(0, 2, proj, 0)

    def norm(i, _):
        ls = pl.multiple_of(i * 256, 256)
        y2[:, pl.ds(ls, 256)] = normed(r[:, pl.ds(ls, 256)], g_ref[...], c_ref[...])
        return 0

    lax.fori_loop(0, nb, norm, 0)

    @pl.when(first)
    def _():
        load_b.wait()

    def up(i, _):
        for j in range(4):
            @pl.when(first & (i == j))
            def _(j=j):
                ups[j].wait()
                if j < 2:
                    ups[j + 2].start()
                elif j == 2:
                    load_2.start()
        ms = pl.multiple_of(i * tile, tile)
        z = dot(w1[pl.ds(ms, tile), :], y2[...]) + widen(b1[pl.ds(ms, tile), :], lanes)
        hh[pl.ds(ms, tile), :] = gelu_of_half(z).astype(BF16)
        return 0

    lax.fori_loop(0, 4, up, 0)
    for pull, push in moves:
        pull.wait()
        push.start()

    @pl.when(first)
    def _():
        load_2.wait()

    def down(i, _):
        ls = pl.multiple_of(i * DOWN, DOWN)
        t = dot(w2[...], hh[:, pl.ds(ls, DOWN)]) + widen(b2[...], DOWN) + r[:, pl.ds(ls, DOWN)]
        t = t.astype(BF16).T
        step = DOWN // 256
        for j in range(nb // step):
            @pl.when(i == j)
            def _():
                for q in range(step):
                    outs[j * step + q][0] = t[q * 256:(q + 1) * 256]
        return 0

    lax.fori_loop(0, lanes // DOWN, down, 0)
    for _, push in moves:
        push.wait()


def mlp(att, xs, at, ks, wo, bo, g, c, w1, b1, w2, b2, idx=None, parts=(), slots=(), shape=None):
    n, d, _ = att.shape
    f = w2.shape[1]
    nb = len(ks)
    lanes = nb * 256
    half = ks[0] // nb
    band = pl.BlockSpec((1, d, 256), lambda i: (i + at, 0, 0))
    extra = [idx, *parts] if parts else []
    total = sum(p.shape[0] for p in parts)
    room = [pltpu.VMEM((total, 256, d), BF16), pltpu.SemaphoreType.DMA((2, len(parts)))] if parts else []
    return pl.pallas_call(
        functools.partial(mlp_kernel, nb=nb, slots=slots), grid=(n,),
        in_specs=[pl.BlockSpec((1, d, lanes), lambda i: (i, 0, half))] + [band] * nb + [ANY, whole1(bo), whole1(g), whole1(c), ANY, ANY, ANY, whole1(b2)]
        + ([pl.BlockSpec(memory_space=pltpu.SMEM)] + [ANY] * len(parts) if parts else []),
        out_specs=[pl.BlockSpec((1, 256, d), lambda i: (i, 0, 0))] * nb + ([ANY] if parts else []),
        out_shape=[jax.ShapeDtypeStruct((n, 256, d), BF16)] * nb + ([shape] if parts else []),
        scratch_shapes=[pltpu.VMEM((d, lanes), F32), pltpu.VMEM((d, lanes), BF16), pltpu.VMEM((f, lanes), BF16),
                        pltpu.VMEM((d, d), BF16), pltpu.VMEM((f, d), BF16), pltpu.VMEM((f, 128), F32), pltpu.VMEM((d, f), BF16),
                        pltpu.SemaphoreType.DMA((7,))] + room,
        name="mlp",
        cost_estimate=pl.CostEstimate(flops=n * nb * 6 * 10 ** 9, bytes_accessed=n * 8 * MIB + 23 * MIB, transcendentals=0),
        compiler_params=pltpu.CompilerParams(vmem_limit_bytes=63 * MIB),
    )(att, *[xs[k] for k in ks], wo, bo, g, c, w1, b1, w2, b2, *extra)


def flip_kernel(w_ref, o_ref, *, rows):
    at = pl.program_id(0) * w_ref.shape[0] + lax.broadcasted_iota(jnp.int32, w_ref.shape, 0)
    o_ref[...] = jnp.where(at < rows, w_ref[...], jnp.zeros_like(w_ref)).T


def flip(w, full, block):
    rows, d = w.shape
    return pl.pallas_call(
        functools.partial(flip_kernel, rows=rows), grid=(full // block,),
        in_specs=[pl.BlockSpec((block, d), lambda i: (i, 0))],
        out_specs=pl.BlockSpec((d, block), lambda i: (0, i)),
        out_shape=jax.ShapeDtypeStruct((d, full), BF16), name="flip",
        cost_estimate=pl.CostEstimate(flops=2 * 10 ** 9, bytes_accessed=20 * MIB, transcendentals=0),
    )(w)


def place_kernel(*refs, slots):
    n = len(slots)
    moves = place_moves(refs[0], refs[1:1 + n], slots, refs[-3], refs[-2], refs[-1])
    for pull, _ in moves:
        pull.start()
    for pull, push in moves:
        pull.wait()
        push.start()
    for _, push in moves:
        push.wait()


def place(idx, parts, slots, out_shape, base=None):
    n = len(parts)
    total = sum(p.shape[0] for p in parts)
    return pl.pallas_call(
        functools.partial(place_kernel, slots=slots),
        in_specs=[pl.BlockSpec(memory_space=pltpu.SMEM)] + [ANY] * (n + (base is not None)),
        out_specs=ANY, out_shape=out_shape, name="place",
        scratch_shapes=[pltpu.VMEM((total,) + parts[0].shape[1:], BF16), pltpu.SemaphoreType.DMA((2, n))],
        input_output_aliases={n + 1: 0} if base is not None else {},
        cost_estimate=pl.CostEstimate(flops=10 ** 9, bytes_accessed=2 * total * 589824, transcendentals=0),
        compiler_params=pltpu.CompilerParams(vmem_limit_bytes=40 * MIB),
    )(idx, *parts, *([base] if base is not None else []))


def column(v, pad=0):
    v = jnp.pad(v, (0, pad)) if pad else v
    return jnp.broadcast_to(v[:, None], (v.shape[0], 128))


def solution(mesh):
    sp = mesh.shape['sp']

    def device_step(images, w_patch, b_patch, pos_embed, ln1_gain, ln1_bias, w_qkv, b_qkv, w_out, b_out, ln2_gain, ln2_bias, w_fc1, b_fc1, w_fc2, b_fc2):
        me = lax.axis_index('sp')
        d = w_patch.shape[3]
        per = images.shape[0] // sp
        planes = jnp.transpose(images, (0, 3, 1, 2))
        x = jnp.arange(512)[:, None]
        o = jnp.arange(512)[None, :]
        px, gx = x % 16, x // 16
        perm = jnp.stack([(o == 128 * (px // 4) + 32 * ((px % 4 + j) % 4) + gx) for j in range(4)]).astype(BF16)
        wp = jnp.transpose(w_patch, (3, 1, 2, 0)).reshape(d, 768)
        pos = pos_embed.T
        bp = column(b_patch)
        wq = jnp.transpose(w_qkv, (1, 2, 3, 0)).reshape(3 * d, d)
        bq = column(b_qkv.reshape(3 * d))
        g1, c1 = column(ln1_gain), column(ln1_bias)
        wo = w_out.reshape(d, d).T
        bo, g2, c2 = column(b_out), column(ln2_gain * 0.5), column(ln2_bias * 0.5)
        pad = 4352 - w_fc1.shape[1]
        w1 = w_fc1.T
        b1 = column(b_fc1 * 0.5, pad)
        w2 = flip(w_fc2, 4352, 2176)
        b2 = column(b_fc2)

        def swap(a, k):
            return lax.ppermute(a, 'sp', [(i, i ^ k) for i in range(sp)]) if k else a

        peers = [me ^ k for k in range(sp)]
        starts = [sum(CHUNKS[:c]) for c in range(len(CHUNKS))]
        got, where = [], []
        for c, n in enumerate(GROUPS):
            begin = sum(GROUPS[:c])
            idx = jnp.stack([p * per + begin for p in peers]).astype(jnp.int32)
            mine = embed(idx, planes, perm, wp, bp, pos, n)
            got.append([swap(a, k) for k, a in enumerate(mine)])
            where += [(c, i) for i in range(n)]
        owner = jnp.stack([p * per for p in peers]).astype(jnp.int32)
        early, slots, res = [], [], None
        shape = jax.ShapeDtypeStruct((images.shape[0], 256, d), BF16)
        last = len(CHUNKS) - 1
        for c, n in enumerate(CHUNKS):
            group, at = where[starts[c]]
            xs = got[group]
            if c:
                own, _ = lax.optimization_barrier((xs[0], res[0]))
                xs = [own] + xs[1:]
            att = attention(xs, at, n, wq, bq, g1, c1)
            if c < last:
                res = mlp(att, xs, at, (0, 1, 2, 3), wo, bo, g2, c2, w1, b1, w2, b2)
                back = [swap(a, k) for k, a in enumerate(res)]
                early += back
                slots += [(k, starts[c]) for k in range(sp)]
            else:
                far = mlp(att, xs, at, (2, 3), wo, bo, g2, c2, w1, b1, w2, b2)
                own, _ = lax.optimization_barrier((xs[0], far[0]))
                near = mlp(att, [own] + xs[1:], at, (0, 1), wo, bo, g2, c2, w1, b1, w2, b2, owner, early, slots, shape)
                back = [near[0], swap(near[1], 1), swap(far[0], 2), swap(far[1], 3)]
        return place(owner, back, [(k, starts[last]) for k in range(sp)], shape, near[2])

    in_specs = (P('dp', 'sp', None, None), P(), P(), P('sp', None)) + (P(),) * 12
    return jax.shard_map(device_step, mesh=mesh, in_specs=in_specs, out_specs=P('dp', 'sp', None), check_vma=False)
```
